256 devices in a mesh: section: 8 (over z), dp: 16 (over x, y_lo, core), tensor: 2 (over y_hi).
Axes of the slice: x: 4, y: 4 (y_hi: 2, y_lo: 2; y = y_hi * 2 + y_lo), z: 8, core: 2. Of those that a mesh axis runs over, the one named last changes fastest.
Arguments:
- activations: bfloat16 [8, 2048, 4096], P('section', 'dp', 'tensor'), may hold values from -32 to 32
- norm_gain: float32 [8, 4096], P('section', 'tensor'), may hold values from 0.5 to 2
- weights: bfloat16 [8, 4096, 1024], P('section', 'tensor'), may hold values from -0.09375 to 0.09375
- cotangent: bfloat16 [8, 2048, 1024], P('section', 'dp'), may hold values from -16 to 16
- top_grad: bfloat16 [2048, 4096], P('dp', 'tensor'), may hold values from -6 to 6
- owner_slot: int32 [8, 2, 13], P('section', 'tensor'), may hold values from 0 to 15, as said below
- sweeps: int32 [8, 2, 16], P('section', 'tensor'), may hold values from 3 to 6
Outputs:
- input_grad: bfloat16 [8, 2048, 4096], P('section', 'dp', 'tensor')
- preconditioned: bfloat16 [8, 4096, 1024], P('section', 'tensor')
The draws below stay inside these ranges and needn't reach their ends.
Inputs may be any that keep to these rules, and one draw needn't show every extreme that they name: For each section and tensor index the 13 entries are distinct; the unit is owned by data replica owner_slot, so a replica owns at most 1 units, and some replica owns exactly 1.
All inputs are finite; a program needn't handle non-finite values.
Results may differ from the reference program's by a relative error of at most 0.035.
Values may be sent and summed in bfloat16 or wider, within the bound.
A program may use at most 128 MiB of HBM per device.

```python
import math
import jax
import jax.numpy as jnp
from jax import lax

D = 4096
KV = 1024
BLOCK = 512
ITERS = 6
TOK_DEV = 128
SECTIONS = 8
TOKENS = 2048
NA = 4
NG = 2
UNITS = 13
CAP = 1
SLOTS = 16
N_DP = 16
N_TENSOR = 2


def draw_activations(key, part):
    key_base = jax.random.fold_in(key, 11)
    key_scale = jax.random.fold_in(key, 12)
    feature_ramp = 1.0 + 2.0 * jnp.arange(D, dtype=jnp.float32) / (D - 1)
    jitter = jnp.exp(jax.random.uniform(key_scale, (SECTIONS, 1, D), minval=-0.3, maxval=0.3))
    values_base = jax.random.normal(key_base, (SECTIONS, TOKENS, D), dtype=jnp.float32)
    return jnp.clip(values_base * feature_ramp * jitter, -32.0, 32.0).astype(jnp.bfloat16)


def draw_cotangent(key, part):
    key_base = jax.random.fold_in(key, 21)
    key_scale = jax.random.fold_in(key, 22)
    column_scale = jnp.exp(jax.random.uniform(key_scale, (SECTIONS, 1, KV), minval=-0.7, maxval=0.7))
    values_base = jax.random.normal(key_base, (SECTIONS, TOKENS, KV), dtype=jnp.float32)
    return jnp.clip(values_base * column_scale, -16.0, 16.0).astype(jnp.bfloat16)


def draw_owner_slot(key, part):
    key_list = jax.random.split(jax.random.fold_in(key, 31), SECTIONS * N_TENSOR)

    def one_table(single_key):
        return jax.random.permutation(single_key, SLOTS)[:UNITS]
    tables = jax.vmap(one_table)(key_list)
    return tables.reshape(SECTIONS, N_TENSOR, UNITS).astype(jnp.int32)


def set_ends(drawn, key, smallest, high):
    index_at = [jax.random.randint(jax.random.fold_in(key, axis), (), 0, length) for axis, length in enumerate(drawn.shape)]
    widest = drawn.shape.index(max(drawn.shape))
    next_to = index_at[:widest] + [(index_at[widest] + 1) % drawn.shape[widest]] + index_at[widest + 1:]
    return drawn.at[tuple(index_at)].set(smallest).at[tuple(next_to)].set(high)


def level_of(key, shape, cuts, least, top_value):
    def one(position, shards_of):
        draws = jax.random.uniform(jax.random.fold_in(jax.random.fold_in(key, 6), position), (shards_of,), jnp.float32, least / len(cuts), top_value / len(cuts))
        return jnp.repeat(jnp.exp(draws), shape[position] // shards_of).reshape((-1,) + (1,) * (len(shape) - position - 1))

    gain = one(*cuts[0])
    for cut in cuts[1:]:
        gain = gain * one(*cut)
    return gain


def noise(rng, extent, scale, limit, shards=(), kind=jnp.bfloat16):
    values = jax.random.normal(rng, extent, jnp.float32) * scale
    if len(shards) > 0:
        values = level_of(rng, extent, shards, -0.22, 0.18) * values
    return jnp.clip(values, min=-limit, max=limit).astype(kind)


def setup_inputs(seed: int = 0) -> dict:
    seeds = jax.random.split(jax.random.key(seed), 8)
    activations = draw_activations(jax.random.fold_in(seeds[7], 71), 0)
    norm_gain = jnp.clip(jnp.exp(math.log(2.0) - 1.3862944 * jax.random.uniform(seeds[1], (SECTIONS, D), jnp.float32) ** level_of(seeds[1], (SECTIONS, D), ((0, 8), (1, 2)), -0.2, 0.2)), 0.5, 2.0)
    weights = noise(seeds[2], (SECTIONS, D, KV), D ** -0.5, 0.09375, ((0, 8), (1, 2)))
    cotangent = draw_cotangent(jax.random.fold_in(seeds[7], 71), 0)
    top_grad = noise(seeds[4], (TOKENS, D), 1.0, 6.0, ((0, 16), (1, 2)))
    owner_slot = draw_owner_slot(jax.random.fold_in(seeds[7], 71), 0)
    sweeps = set_ends(jax.random.randint(seeds[6], (SECTIONS, N_TENSOR, N_DP), ITERS - 3, ITERS + 1), jax.random.fold_in(seeds[6], 1), ITERS - 3, ITERS).astype(jnp.int32)
    return {"activations": activations, "norm_gain": norm_gain, "weights": weights, "cotangent": cotangent, "top_grad": top_grad, "owner_slot": owner_slot, "sweeps": sweeps}


EPSILON = 1e-05
DAMPING = 0.05
HIGHEST_PREC = lax.Precision.HIGHEST

def rounded(values):
    return lax.optimization_barrier(values.astype(jnp.bfloat16)).astype(jnp.float32)

def newton_schulz(matrices, limits):
    order_size = matrices.shape[-1]
    identity = jnp.eye(order_size, dtype=jnp.float32)
    frobenius = jnp.sqrt(lax.optimization_barrier(jnp.sum(matrices * matrices, axis=(1, 2))))
    approx = identity[None] / frobenius[:, None, None]
    for each_sweep in range(ITERS):
        product = jnp.einsum('cij,cjk->cik', matrices, approx, precision=HIGHEST_PREC)
        update = jnp.einsum('cij,cjk->cik', approx, 2.0 * identity[None] - product, precision=HIGHEST_PREC)
        approx = jnp.where((each_sweep < limits)[:, None, None], update, approx)
    return approx

def reference(activations, norm_gain, weights, cotangent, top_grad, owner_slot, sweeps):
    identity = jnp.eye(BLOCK, dtype=jnp.float32)
    terms_all = []
    pre_blocks = []
    for section_index in range(SECTIONS):
        inputs = activations[section_index].astype(jnp.float32)
        gain_row = norm_gain[section_index]
        squares = lax.optimization_barrier(jnp.sum(inputs * inputs, axis=1))
        inverse_rms = lax.rsqrt(squares / D + EPSILON)
        normed = (inputs * inverse_rms[:, None] * gain_row[None]).astype(jnp.bfloat16)
        upstream_v = cotangent[section_index]
        upstream = lax.dot_general(upstream_v, weights[section_index], (((1,), (1,)), ((), ())), preferred_element_type=jnp.float32)
        scaled = upstream * gain_row[None]
        inner_sum = lax.optimization_barrier(jnp.sum(scaled * inputs, axis=1))
        terms_all.append(inverse_rms[:, None] * scaled - inputs * (inverse_rms ** 3 * inner_sum / D)[:, None])
        normed_parts = normed.reshape(N_DP, TOK_DEV, D // BLOCK, BLOCK).astype(jnp.float32)
        value_parts = upstream_v.reshape(N_DP, TOK_DEV, NG, BLOCK).astype(jnp.float32)
        feature_sum = lax.optimization_barrier(jnp.sum(rounded(jnp.einsum('rtia,rtib->riab', normed_parts, normed_parts)), axis=0))
        value_sum = lax.optimization_barrier(jnp.sum(rounded(jnp.einsum('rtja,rtjb->rjab', value_parts, value_parts)), axis=0))
        grad_sum = lax.optimization_barrier(jnp.sum(rounded(jnp.einsum('rtia,rtjb->rijab', normed_parts, value_parts)), axis=0))
        feature_limits = []
        value_limits = []
        for half_index in range(N_TENSOR):
            counts = sweeps[section_index, half_index]
            owners = (owner_slot[section_index, half_index, :NA + 1] // CAP).astype(jnp.int32)
            unit_limits = jnp.take(counts, owners)
            feature_limits.append(unit_limits[:NA])
            value_limits.append(unit_limits[NA:NA + 1])
        feature_inv = newton_schulz(feature_sum / TOKENS + DAMPING * identity[None], jnp.concatenate(feature_limits)).astype(jnp.bfloat16)
        value_inv = newton_schulz(value_sum / TOKENS + DAMPING * identity[None], jnp.concatenate(value_limits)).astype(jnp.bfloat16)
        grad_round = grad_sum.astype(jnp.bfloat16)
        left_part = jnp.einsum('iab,ijbc->ijac', feature_inv.astype(jnp.float32), grad_round.astype(jnp.float32)).astype(jnp.bfloat16)
        result = jnp.einsum('ijac,jcd->iajd', left_part.astype(jnp.float32), value_inv.astype(jnp.float32)).astype(jnp.bfloat16)
        pre_blocks.append(result.reshape(D, KV))
    terms_stack = jnp.stack(terms_all)
    inclusive = jnp.flip(jnp.cumsum(jnp.flip(terms_stack, 0), axis=0), 0)
    input_grad = (top_grad.astype(jnp.float32)[None] + inclusive).astype(jnp.bfloat16)
    return (input_grad, jnp.stack(pre_blocks))
```

```python
import functools

import jax
import jax.numpy as jnp
from jax import lax
from jax.experimental import pallas as pl
from jax.experimental.pallas import tpu as pltpu
from jax.sharding import PartitionSpec as P

BLOCK = 512
ITERS = 6
EPSILON = 1e-05
DAMPING = 0.05
NX = 4
NF = 4
CHUNKS = 8
MESH = pl.DeviceIdType.MESH
F32 = jnp.float32
BF16 = jnp.bfloat16


def remote(src, dst, send, recv, device):
    return pltpu.make_async_remote_copy(
        src_ref=src,
        dst_ref=dst,
        send_sem=send,
        recv_sem=recv,
        device_id=device,
        device_id_type=MESH,
    )


def dot_tn(a, b):
    return lax.dot_general(a, b, (((0,), (0,)), ((), ())), preferred_element_type=F32)


def dot_nt(a, b):
    return lax.dot_general(a, b, (((1,), (1,)), ((), ())), preferred_element_type=F32)


def dot_nn(a, b):
    return lax.dot_general(a, b, (((1,), (0,)), ((), ())), preferred_element_type=F32)


def kernel(
    sections,
    tokens,
    owner,
    sweeps,
    act,
    gain,
    weights,
    cot,
    top,
    grad_out,
    pre_out,
    xv,
    cv,
    wv,
    tv,
    scaled,
    nsend,
    nbuf,
    cbuf,
    ee,
    xx,
    eb,
    gb,
    vb,
    pv,
    sqs,
    sqr,
    ins,
    inr,
    inv_v,
    coef_v,
    lim,
    zsend,
    zrecv,
    og,
    load_sem,
    cs_sem,
    cr_sem,
    ns_sem,
    nf_sem,
    nd_sem,
    nr_sem,
    small_s,
    small_r,
    zs_sem,
    zr_sem,
    gv_s,
    gv_r,
    as_sem,
    ar_sem,
    wr_sem,
    og_sem,
):
    s = lax.axis_index("section")
    r = lax.axis_index("dp")
    t = lax.axis_index("tensor")
    x = r // 4
    y = (r // 2) % 2
    c = r % 2
    tok = xv.shape[1]
    cw = xv.shape[2]
    full = NF * BLOCK * 2

    def at(dx, dy, core):
        return (((x + dx) % NX) * 2 + (y + dy) % 2) * 2 + core

    def dp(index):
        return {"dp": index}

    loads = []
    for j in range(2):
        loads.append(
            pltpu.make_async_copy(
                cot.at[0, :, pl.ds(j * BLOCK, BLOCK)], cv.at[j], load_sem.at[j]
            )
        )
    for k in range(CHUNKS):
        loads.append(
            pltpu.make_async_copy(
                act.at[0, :, pl.ds(k * cw, cw)], xv.at[k], load_sem.at[2 + k]
            )
        )
    loads.append(pltpu.make_async_copy(weights.at[0], wv, load_sem.at[2 + CHUNKS]))
    for k in range(CHUNKS):
        loads.append(
            pltpu.make_async_copy(
                top.at[:, pl.ds(k * cw, cw)], tv.at[k], load_sem.at[3 + CHUNKS + k]
            )
        )
    for load in loads:
        load.start()

    barrier = pltpu.get_barrier_semaphore()
    for k in range(1, 16):
        pl.semaphore_signal(barrier, inc=1, device_id=dp((r + k) % 16), device_id_type=MESH)
    pl.semaphore_signal(barrier, inc=1, device_id={"tensor": 1 - t}, device_id_type=MESH)
    for k in (1, sections - 1):
        pl.semaphore_signal(
            barrier, inc=1, device_id={"section": (s + k) % sections}, device_id_type=MESH
        )

    for k in range(CHUNKS):
        loads[2 + k].wait()

    def square_step(k, total):
        v = xv[k].astype(F32)
        v = v * v
        for h in range(cw // 128):
            total = total + v[:, h * 128 : (h + 1) * 128]
        return total

    squares = lax.fori_loop(0, CHUNKS, square_step, jnp.zeros((tok, 128), F32))
    squares = jnp.broadcast_to(jnp.sum(squares, axis=1, keepdims=True), (tok, 128))
    sqs[pl.ds(0, tok), :] = squares
    own_limit = sweeps[0, 0, owner[0, 0, NF]].astype(F32)
    sqs[pl.ds(tok, 8), :] = jnp.full((8, 128), own_limit, F32)
    loads[0].wait()
    loads[1].wait()
    pl.semaphore_wait(barrier, 18)
    partner = {"tensor": 1 - t}
    squares_copy = remote(sqs, sqr, small_s.at[0], small_r.at[0], partner)
    squares_copy.start()

    value_core = c == 0
    feature_core = c == 1

    def c_slot(index):
        return cbuf.at[pl.ds(pl.multiple_of(index * tok, tok), tok), :]

    def n_slot(index):
        return nbuf.at[pl.ds(pl.multiple_of(index * tok, tok), tok), :]

    def c_send(k):
        if k == 0:
            return remote(cv.at[1 - y], c_slot(r), cs_sem.at[0], cr_sem.at[r], dp(at(0, 1, 0)))
        dx = (None, 1, 3, 2)[k]
        return remote(cv.at[y], c_slot(r), cs_sem.at[k], cr_sem.at[r], dp(at(dx, 0, 0)))

    c_home = remote(cv.at[y], c_slot(r), cs_sem.at[4], cr_sem.at[r], dp(at(0, 0, 0)))
    for k in range(4):
        c_send(k).start()

    @pl.when(feature_core)
    def _():
        c_home.start()

    @pl.when(value_core)
    def _():
        c_slot(r)[...] = cv[y]

    loads[2 + CHUNKS].wait()

    def upstream_step(k, total):
        rows = pl.ds(pl.multiple_of(k * cw, cw), cw)
        up = dot_nt(cv[0], wv[rows, pl.ds(0, BLOCK)]) + dot_nt(cv[1], wv[rows, pl.ds(BLOCK, BLOCK)])
        up = up * gain[0:1, pl.ds(pl.multiple_of(k * cw, cw), cw)]
        scaled[k] = up
        up = up * xv[k].astype(F32)
        for h in range(cw // 128):
            total = total + up[:, h * 128 : (h + 1) * 128]
        return total

    inner = lax.fori_loop(0, CHUNKS, upstream_step, jnp.zeros((tok, 128), F32))
    inner = jnp.broadcast_to(jnp.sum(inner, axis=1, keepdims=True), (tok, 128))
    ins[...] = inner
    inner_copy = remote(ins, inr, small_s.at[1], small_r.at[1], partner)
    inner_copy.start()

    squares_copy.wait_recv()
    inverse = lax.rsqrt((sqs[pl.ds(0, tok), :] + sqr[pl.ds(0, tok), :]) / full + EPSILON)
    inv_v[...] = inverse

    def n_send(k):
        dx = (1, 3, 2, 0)[k]
        return remote(
            nsend.at[(x + dx) % NX], n_slot(r), ns_sem.at[k], nr_sem.at[r], dp(at(dx, 0, 1))
        )

    half = BLOCK // cw

    def norm_block(i):
        for h in range(BLOCK // 128):
            k = i * half + h * 128 // cw
            lane = (h * 128) % cw
            row = gain[0:1, pl.ds(pl.multiple_of(i * BLOCK + h * 128, 128), 128)]
            v = xv[k, :, lane : lane + 128].astype(F32) * inverse * row
            nsend[i, :, h * 128 : (h + 1) * 128] = v.astype(BF16)

    for k in range(3):
        norm_block((x + (1, 3, 2)[k]) % NX)
        n_send(k).start()
    norm_block(x)

    @pl.when(value_core)
    def _():
        n_send(3).start()

    @pl.when(feature_core)
    def _():
        n_slot(r)[...] = nsend[x]

    inner_copy.wait_recv()
    coef_v[...] = inverse * inverse * inverse * (ins[...] + inr[...]) / full
    for k in range(CHUNKS):
        loads[3 + CHUNKS + k].wait()

    def z_copy(chunk):
        return remote(
            zsend.at[chunk],
            zrecv.at[chunk],
            zs_sem.at[chunk],
            zr_sem.at[chunk],
            {"section": (s + sections - 1) % sections},
        )

    def og_copy(chunk):
        columns = pl.ds(pl.multiple_of(chunk * cw, cw), cw)
        return pltpu.make_async_copy(
            og.at[chunk], grad_out.at[0, :, columns], og_sem.at[chunk]
        )

    def z_slot(k):
        chunk = k - (sections - 1 - s)

        @pl.when((chunk >= 0) & (chunk < CHUNKS))
        def _():
            @pl.when(s < sections - 1)
            def _():
                z_copy(chunk).wait_recv()

            @pl.when(s == sections - 1)
            def _():
                zrecv[chunk] = jnp.zeros((tok, cw), BF16)

            for h in range(cw // 128):
                lanes = slice(h * 128, (h + 1) * 128)
                term = inv_v[...] * scaled[chunk, :, lanes] - xv[chunk, :, lanes].astype(F32) * coef_v[...]
                term = term + zrecv[chunk, :, lanes].astype(F32)
                zsend[chunk, :, lanes] = term.astype(BF16)
                og[chunk, :, lanes] = (tv[chunk, :, lanes].astype(F32) + term).astype(BF16)

            @pl.when(s > 0)
            def _():
                z_copy(chunk).start()

            og_copy(chunk).start()

    slots = sections - 1 + CHUNKS
    ee[...] = jnp.zeros((BLOCK, BLOCK), F32)

    def n_forward(k, core):
        dx = k + k // 2 - 2 * (k // 3)
        index = at(dx, 0, core)
        return remote(
            n_slot(index), n_slot(index), nf_sem.at[2 * k + core], nr_sem.at[index], dp(at(0, 1, 1))
        )

    def n_home(k, core):
        dx = k % 4 + (k % 4) // 2 - 2 * ((k % 4) // 3)
        index = at(dx, k // 4, core)
        return remote(
            n_slot(index), n_slot(index), nd_sem.at[2 * k + core], nr_sem.at[index], dp(at(0, 0, 0))
        )

    @pl.when(feature_core)
    def _():
        def step(k, carry):
            for core in (1, 0):
                if core == 0:
                    n_home(k, core).wait_recv()
                else:

                    @pl.when(k > 0)
                    def _():
                        n_home(k, core).wait_recv()

                @pl.when(k < 4)
                def _():
                    n_forward(k % 4, core).start()

                n_home(k, core).start()
            dx = k % 4 + (k % 4) // 2 - 2 * ((k % 4) // 3)
            index = at(dx, k // 4, 0)
            rows = nbuf[pl.ds(pl.multiple_of(index * tok, 2 * tok), 2 * tok), :]
            ee[...] = ee[...] + dot_tn(rows, rows)

            @pl.when(k >= 3)
            def _():
                z_slot(k - 3)

            return carry

        lax.fori_loop(0, 8, step, 0)
        limit = sweeps[0, 0, owner[0, 0, x]].astype(F32)
        lim[...] = jnp.full((8, BLOCK), limit, F32)

    def c_place(k):
        high = (k + 6) // 8
        m = (k - 2) * high
        dx = high * (1 + 2 * (m % 3) - 3 * ((m % 3) // 2))
        dy = high * (m // 3) + (1 - high) * k
        return dx, dy

    def c_forward(core, k):
        index = at(0, 1, core)
        dx = (1, 3, 2)[k]
        return remote(
            c_slot(index), c_slot(index), cs_sem.at[5 + 3 * core + k], cr_sem.at[index], dp(at(dx, 0, 0))
        )

    def c_arrived(index):
        return remote(c_slot(index), c_slot(index), cs_sem.at[0], cr_sem.at[index], dp(at(1, 0, 0)))

    @pl.when(value_core)
    def _():
        def step(k, carry):
            dx, dy = c_place(k)
            for core in (0, 1):
                if core == 1:
                    c_arrived(at(dx, dy, core)).wait_recv()
                else:

                    @pl.when(k > 0)
                    def _():
                        c_arrived(at(dx, dy, core)).wait_recv()

                @pl.when(k == 1)
                def _():
                    for q in range(3):
                        c_forward(core, q).start()

            rows = cbuf[pl.ds(pl.multiple_of(at(dx, dy, 0) * tok, 2 * tok), 2 * tok), :]
            ee[...] = ee[...] + dot_tn(rows, rows)

            @pl.when(k >= 3)
            def _():
                z_slot(k - 3)

            return carry

        lax.fori_loop(0, 8, step, 0)
        other = jnp.max(sqr[pl.ds(tok, 8), :], axis=0, keepdims=True)
        own = jnp.full((1, 128), own_limit, F32)
        limit = jnp.where(y == t, own, other)
        for h in range(BLOCK // 128):
            lim[:, h * 128 : (h + 1) * 128] = jnp.broadcast_to(limit, (8, 128))

    diagonal = lax.broadcasted_iota(jnp.int32, (BLOCK, BLOCK), 0) == lax.broadcasted_iota(
        jnp.int32, (BLOCK, BLOCK), 1
    )
    matrix = ee[...] / tokens + jnp.where(diagonal, DAMPING, 0.0)
    norm = lax.rsqrt(jnp.sum(jnp.sum(matrix * matrix, axis=0, keepdims=True), axis=1, keepdims=True))
    ee[...] = matrix * norm
    xx[...] = jnp.where(diagonal, 1.0, 0.0) * norm

    def sweep(k, carry):
        eb[...] = ee[...].astype(BF16)

        @pl.when(k > 0)
        def _():
            old = xx[...]
            new = 2.0 * old - dot_nn(old.astype(BF16), eb[...])
            xx[...] = jnp.where(lim[0:1, :] > k.astype(F32), new, old)

        @pl.when(k == 0)
        def _():
            xx[...] = 2.0 * xx[...] - ee[...] * norm

        @pl.when(k < ITERS - 1)
        def _():
            e = ee[...]
            ee[...] = 2.0 * e - dot_nn(eb[...], eb[...])
            z_slot(k + 5)

        return carry

    lax.fori_loop(0, ITERS, sweep, 0)
    eb[...] = xx[...].astype(BF16)

    v_copy = remote(eb, vb, gv_s.at[0], gv_r.at[0], dp(at(0, 0, 1)))
    g_copy = remote(gb, gb, gv_s.at[1], gv_r.at[1], dp(at(0, 0, 1)))

    @pl.when(value_core)
    def _():
        v_copy.start()
        xx[...] = jnp.zeros((BLOCK, BLOCK), F32)

        def step(k, carry):
            dx = k % 4 + (k % 4) // 2 - 2 * ((k % 4) // 3)
            for core in (1, 0):
                n_home(k, core).wait_recv()
            rows = pl.ds(pl.multiple_of(at(dx, k // 4, 0) * tok, 2 * tok), 2 * tok)
            xx[...] = xx[...] + dot_tn(nbuf[rows, :], cbuf[rows, :])
            return carry

        lax.fori_loop(0, 8, step, 0)
        gb[...] = xx[...].astype(BF16)
        g_copy.start()

    rows_q = BLOCK // 4

    def piece(dx, dy, q):
        return (((x + dx) % NX) * 2 + (y + dy) % 2) * 4 + q

    def out_at(dx, dy, q):
        i = (x + dx) % NX
        j = (y + dy) % 2
        return pre_out.at[
            0,
            pl.ds(pl.multiple_of(i * BLOCK + q * rows_q, rows_q), rows_q),
            pl.ds(pl.multiple_of(j * BLOCK, BLOCK), BLOCK),
        ]

    def to(dx, dy, q, n, device):
        index = piece(dx, dy, q)
        return remote(pv.at[index], pv.at[index], as_sem.at[n], ar_sem.at[index], dp(device))

    def across(dx, dy, q, n):
        index = piece(dx, dy, q)
        return remote(
            pv.at[index], out_at(dx, dy, q), as_sem.at[n], ar_sem.at[index], dp(at(0, 0, 1 - c))
        )

    def arrived(dx, dy, q):
        return to(dx, dy, q, 0, at(0, 0, 1 - c))

    def write(dx, dy, q, n):
        return pltpu.make_async_copy(pv.at[piece(dx, dy, q)], out_at(dx, dy, q), wr_sem.at[n])

    def run(events, my_core):
        started = []
        writes = []
        n = 0
        for number, (dx, dy, q, arrives, goes) in enumerate(events):
            if arrives:
                arrived(dx, dy, q).wait_recv()
            for where in goes:
                if where == "home":
                    copy = to(dx, dy, q, n, at(0, 0, 1 - my_core))
                elif where == "across":
                    copy = across(dx, dy, q, n)
                else:
                    copy = to(dx, dy, q, n, at(*where))
                copy.start()
                started.append(copy)
                n += 1
            out = write(dx, dy, q, number)
            out.start()
            writes.append(out)
            yield
        for dx, dy, q in [
            (dx, dy, q)
            for dy in range(2)
            for dx in (0, 1, 3, 2)
            for q in ((2, 3) if my_core == 1 else (0, 1))
            if my_core == 0 or (dx, dy) != (0, 0)
        ]:
            index = piece(dx, dy, q)
            remote(
                pv.at[index], out_at(dx, dy, q), as_sem.at[0], ar_sem.at[index], dp(at(0, 0, 1 - c))
            ).wait_recv()
        for copy in started:
            copy.wait_send()
        for out in writes:
            out.wait()

    @pl.when(feature_core)
    def _():
        right, left, up = (1, 0, 1), (3, 0, 1), (0, 1, 1)
        g_copy.wait_recv()
        v_copy.wait_recv()
        events = []
        for q in (0, 2, 1, 3):
            if q < 2:
                events.append((0, 0, q, False, (right, left, up, "across")))
            else:
                events.append((0, 0, q, False, ((0, 1, 0), "home")))
        events += [
            (3, 0, 0, True, (right, up, "across")),
            (1, 0, 1, True, (left, up, "across")),
            (0, 1, 0, True, ("across",)),
            (3, 0, 1, True, (up, "across")),
            (1, 0, 0, True, (up, "across")),
            (0, 1, 1, True, ("across",)),
            (2, 0, 0, True, (up, "across")),
            (2, 0, 1, True, (up, "across")),
            (3, 1, 0, True, ("across",)),
            (1, 1, 1, True, ("across",)),
            (3, 1, 1, True, ("across",)),
            (1, 1, 0, True, ("across",)),
            (2, 1, 0, True, ("across",)),
            (2, 1, 1, True, ("across",)),
        ]
        steps = run(events, 1)
        for q in (0, 2, 1, 3):
            rows = slice(q * rows_q, (q + 1) * rows_q)
            first = dot_nn(eb[rows, :], gb[...]).astype(BF16)
            pv[piece(0, 0, q)] = dot_nn(first, vb[...]).astype(BF16)
            next(steps)
        done = 4
        for k in range(10, slots):
            z_slot(k)
            for _ in range(3):
                if done < len(events):
                    next(steps)
                    done += 1
        for _ in steps:
            pass

    @pl.when(value_core)
    def _():
        right, left = (1, 0, 0), (3, 0, 0)
        events = [
            (0, 0, 2, True, (right, left)),
            (0, 1, 2, True, (right, left, "across")),
            (0, 0, 3, True, (left, right)),
            (0, 1, 3, True, (left, right, "across")),
            (3, 0, 2, True, (right, "across")),
            (1, 0, 3, True, (left, "across")),
            (3, 1, 2, True, (right, "across")),
            (1, 1, 3, True, (left, "across")),
            (3, 0, 3, True, ("across",)),
            (1, 0, 2, True, ("across",)),
            (3, 1, 3, True, ("across",)),
            (1, 1, 2, True, ("across",)),
            (2, 0, 2, True, ("across",)),
            (2, 0, 3, True, ("across",)),
            (2, 1, 2, True, ("across",)),
            (2, 1, 3, True, ("across",)),
        ]
        steps = run(events, 0)
        done = 0
        for k in range(10, slots):
            z_slot(k)
            for _ in range(3):
                if done < len(events):
                    next(steps)
                    done += 1
        for _ in steps:
            pass

    squares_copy.wait_send()
    inner_copy.wait_send()
    for k in range(4):
        c_send(k).wait_send()
    for k in range(3):
        n_send(k).wait_send()

    @pl.when(feature_core)
    def _():
        c_home.wait_send()

        def ended(k, carry):
            for core in (1, 0):
                n_home(k, core).wait_send()

                @pl.when(k < 4)
                def _():
                    n_forward(k % 4, core).wait_send()

            return carry

        lax.fori_loop(0, 8, ended, 0)

    @pl.when(value_core)
    def _():
        n_send(3).wait_send()
        for core in range(2):
            for k in range(3):
                c_forward(core, k).wait_send()
        v_copy.wait_send()
        g_copy.wait_send()

    def chain_ended(chunk, carry):
        @pl.when(s > 0)
        def _():
            z_copy(chunk).wait_send()

        og_copy(chunk).wait()
        return carry

    lax.fori_loop(0, CHUNKS, chain_ended, 0)


def on_device(sections, tokens, activations, norm_gain, weights, cotangent, top_grad, owner_slot, sweeps):
    tok, half_width = activations.shape[1:]
    value_width = weights.shape[2]
    cw = half_width // CHUNKS
    vmem = functools.partial(pltpu.VMEM)
    dma = pltpu.SemaphoreType.DMA
    anywhere = pl.BlockSpec(memory_space=pl.ANY)
    smem = pl.BlockSpec(memory_space=pltpu.SMEM)
    return pl.pallas_call(
        functools.partial(kernel, sections, tokens),
        out_shape=(
            jax.ShapeDtypeStruct((1, tok, half_width), BF16),
            jax.ShapeDtypeStruct((1, half_width, value_width), BF16),
        ),
        in_specs=[
            smem,
            smem,
            anywhere,
            pl.BlockSpec(memory_space=pltpu.VMEM),
            anywhere,
            anywhere,
            anywhere,
        ],
        out_specs=(anywhere, anywhere),
        scratch_shapes=[
            vmem((CHUNKS, tok, cw), BF16),
            vmem((2, tok, BLOCK), BF16),
            vmem((half_width, value_width), BF16),
            vmem((CHUNKS, tok, cw), BF16),
            vmem((CHUNKS, tok, cw), F32),
            vmem((NF, tok, BLOCK), BF16),
            vmem((tok * 16, BLOCK), BF16),
            vmem((tok * 16, BLOCK), BF16),
            vmem((BLOCK, BLOCK), F32),
            vmem((BLOCK, BLOCK), F32),
            vmem((BLOCK, BLOCK), BF16),
            vmem((BLOCK, BLOCK), BF16),
            vmem((BLOCK, BLOCK), BF16),
            vmem((32, BLOCK // 4, BLOCK), BF16),
            vmem((tok + 8, 128), F32),
            vmem((tok + 8, 128), F32),
            vmem((tok, 128), F32),
            vmem((tok, 128), F32),
            vmem((tok, 128), F32),
            vmem((tok, 128), F32),
            vmem((8, BLOCK), F32),
            vmem((CHUNKS, tok, cw), BF16),
            vmem((CHUNKS, tok, cw), BF16),
            vmem((CHUNKS, tok, cw), BF16),
            dma((3 + 2 * CHUNKS,)),
            dma((11,)),
            dma((16,)),
            dma((4,)),
            dma((8,)),
            dma((16,)),
            dma((16,)),
            dma((2,)),
            dma((2,)),
            dma((CHUNKS,)),
            dma((CHUNKS,)),
            dma((2,)),
            dma((2,)),
            dma((40,)),
            dma((32,)),
            dma((18,)),
            dma((CHUNKS,)),
        ],
        compiler_params=pltpu.CompilerParams(
            collective_id=0, has_side_effects=True, vmem_limit_bytes=60000 * 1024
        ),
        name="kfac",
    )(owner_slot, sweeps, activations, norm_gain, weights, cotangent, top_grad)


def solution(mesh):
    sections = mesh.shape["section"]
    placed = (
        P("section", "dp", "tensor"),
        P("section", "tensor"),
        P("section", "tensor", None),
        P("section", "dp", None),
        P("dp", "tensor"),
        P("section", "tensor", None),
        P("section", "tensor", None),
    )

    def step(activations, *rest):
        return on_device(sections, activations.shape[1] * 16, activations, *rest)

    return jax.shard_map(
        step,
        mesh=mesh,
        in_specs=placed,
        out_specs=(P("section", "dp", "tensor"), P("section", "tensor", None)),
        check_vma=False,
    )
```

```python
import functools

import jax
import jax.numpy as jnp
from jax import lax
from jax.experimental import pallas as pl
from jax.experimental.pallas import tpu as pltpu
from jax.sharding import PartitionSpec as P

BLOCK = 512
ITERS = 6
EPSILON = 1e-05
DAMPING = 0.05
NX = 4
NF = 4
CHUNKS = 8
MESH = pl.DeviceIdType.MESH
F32 = jnp.float32
BF16 = jnp.bfloat16


def remote(src, dst, send, recv, device):
    return pltpu.make_async_remote_copy(
        src_ref=src,
        dst_ref=dst,
        send_sem=send,
        recv_sem=recv,
        device_id=device,
        device_id_type=MESH,
    )


def as_row(partial):
    return jnp.broadcast_to(jnp.sum(partial.T, axis=0, keepdims=True), (8, partial.shape[0]))


def as_column(row):
    return jnp.broadcast_to(row, (row.shape[1], row.shape[1])).T


def dot_tn(a, b):
    return lax.dot_general(a, b, (((0,), (0,)), ((), ())), preferred_element_type=F32)


def dot_nt(a, b):
    return lax.dot_general(a, b, (((1,), (1,)), ((), ())), preferred_element_type=F32)


def dot_nn(a, b):
    return lax.dot_general(a, b, (((1,), (0,)), ((), ())), preferred_element_type=F32)


def kernel(
    sections,
    tokens,
    owner,
    sweeps,
    act,
    gain,
    weights,
    cot,
    top,
    og,
    pv,
    xv,
    cv,
    wv,
    tv,
    scaled,
    nsend,
    nbuf,
    cbuf,
    ee,
    xx,
    eb,
    gb,
    vb,
    sqs,
    sqr,
    ins,
    inr,
    inv_v,
    coef_v,
    lim,
    zsend,
    zrecv,
    load_sem,
    cs_sem,
    cr_sem,
    ns_sem,
    nf_sem,
    nd_sem,
    nr_sem,
    small_s,
    small_r,
    zs_sem,
    zr_sem,
    gv_s,
    gv_r,
    as_sem,
    ar_sem,
):
    s = lax.axis_index("section")
    r = lax.axis_index("dp")
    t = lax.axis_index("tensor")
    x = r // 4
    y = (r // 2) % 2
    c = r % 2
    tok = xv.shape[1]
    cw = xv.shape[2]
    full = NF * BLOCK * 2

    def at(dx, dy, core):
        return (((x + dx) % NX) * 2 + (y + dy) % 2) * 2 + core

    def dp(index):
        return {"dp": index}

    loads = []
    for j in range(2):
        loads.append(
            pltpu.make_async_copy(
                cot.at[0, :, pl.ds(j * BLOCK, BLOCK)], cv.at[j], load_sem.at[j]
            )
        )
    for k in range(CHUNKS):
        loads.append(
            pltpu.make_async_copy(
                act.at[0, :, pl.ds(k * cw, cw)], xv.at[k], load_sem.at[2 + k]
            )
        )
    loads.append(pltpu.make_async_copy(weights.at[0], wv, load_sem.at[2 + CHUNKS]))
    for k in range(CHUNKS):
        loads.append(
            pltpu.make_async_copy(
                top.at[:, pl.ds(k * cw, cw)], tv.at[k], load_sem.at[3 + CHUNKS + k]
            )
        )
    for load in loads:
        load.start()

    barrier = pltpu.get_barrier_semaphore()
    for k in range(1, 16):
        pl.semaphore_signal(barrier, inc=1, device_id=dp((r + k) % 16), device_id_type=MESH)
    pl.semaphore_signal(barrier, inc=1, device_id={"tensor": 1 - t}, device_id_type=MESH)

    @pl.when(s < sections - 1)
    def _():
        pl.semaphore_signal(barrier, inc=1, device_id={"section": s + 1}, device_id_type=MESH)

    for k in range(CHUNKS):
        loads[2 + k].wait()

    def square_step(k, total):
        v = xv[k].astype(F32)
        v = v * v
        for h in range(cw // 128):
            total = total + v[:, h * 128 : (h + 1) * 128]
        return total

    squares = lax.fori_loop(0, CHUNKS, square_step, jnp.zeros((tok, 128), F32))
    own_limit = sweeps[0, 0, owner[0, 0, NF]].astype(F32)
    sqs[0:8, :] = as_row(squares)
    sqs[8:16, :] = jnp.full((8, 128), own_limit, F32)
    loads[0].wait()
    loads[1].wait()

    @pl.when(s > 0)
    def _():
        pl.semaphore_wait(barrier, 17)

    @pl.when(s == 0)
    def _():
        pl.semaphore_wait(barrier, 16)

    partner = {"tensor": 1 - t}
    squares_copy = remote(sqs, sqr, small_s.at[0], small_r.at[0], partner)
    squares_copy.start()

    value_core = c == 0
    feature_core = c == 1

    def c_slot(index):
        return cbuf.at[pl.ds(pl.multiple_of(index * tok, tok), tok), :]

    def n_slot(index):
        return nbuf.at[pl.ds(pl.multiple_of(index * tok, tok), tok), :]

    def c_send(k):
        if k == 0:
            return remote(cv.at[1 - y], c_slot(r), cs_sem.at[0], cr_sem.at[r], dp(at(0, 1, 0)))
        dx = (None, 1, 3, 2)[k]
        return remote(cv.at[y], c_slot(r), cs_sem.at[k], cr_sem.at[r], dp(at(dx, 0, 0)))

    c_home = remote(cv.at[y], c_slot(r), cs_sem.at[4], cr_sem.at[r], dp(at(0, 0, 0)))
    for k in range(4):
        c_send(k).start()

    @pl.when(feature_core)
    def _():
        c_home.start()

    @pl.when(value_core)
    def _():
        c_slot(r)[...] = cv[y]

    loads[2 + CHUNKS].wait()

    def upstream_step(k, total):
        rows = pl.ds(pl.multiple_of(k * cw, cw), cw)
        up = dot_nt(cv[0], wv[rows, pl.ds(0, BLOCK)]) + dot_nt(cv[1], wv[rows, pl.ds(BLOCK, BLOCK)])
        up = up * gain[0:1, pl.ds(pl.multiple_of(k * cw, cw), cw)]
        scaled[k] = up
        up = up * xv[k].astype(F32)
        for h in range(cw // 128):
            total = total + up[:, h * 128 : (h + 1) * 128]
        return total

    inner = lax.fori_loop(0, CHUNKS, upstream_step, jnp.zeros((tok, 128), F32))
    ins[...] = as_row(inner)
    inner_copy = remote(ins, inr, small_s.at[1], small_r.at[1], partner)
    inner_copy.start()

    squares_copy.wait_recv()
    inverse_row = lax.rsqrt((sqs[0:1, :] + sqr[0:1, :]) / full + EPSILON)
    inverse = as_column(inverse_row)
    inv_v[...] = inverse

    def n_send(k):
        dx = (1, 3, 2, 0)[k]
        return remote(
            nsend.at[(x + dx) % NX], n_slot(r), ns_sem.at[k], nr_sem.at[r], dp(at(dx, 0, 1))
        )

    half = BLOCK // cw

    def norm_block(i):
        for h in range(BLOCK // 128):
            k = i * half + h * 128 // cw
            lane = (h * 128) % cw
            row = gain[0:1, pl.ds(pl.multiple_of(i * BLOCK + h * 128, 128), 128)]
            v = xv[k, :, lane : lane + 128].astype(F32) * inverse * row
            nsend[i, :, h * 128 : (h + 1) * 128] = v.astype(BF16)

    for k in range(3):
        norm_block((x + (1, 3, 2)[k]) % NX)
        n_send(k).start()
    norm_block(x)

    @pl.when(value_core)
    def _():
        n_send(3).start()

    @pl.when(feature_core)
    def _():
        n_slot(r)[...] = nsend[x]

    def term_ready():
        inner_copy.wait_recv()
        row = lax.rsqrt((sqs[0:1, :] + sqr[0:1, :]) / full + EPSILON)
        coef_v[...] = as_column(row * row * row * (ins[0:1, :] + inr[0:1, :]) / full)
        for k in range(CHUNKS):
            loads[3 + CHUNKS + k].wait()

    def z_copy(chunk):
        return remote(
            zsend.at[chunk],
            zrecv.at[chunk],
            zs_sem.at[chunk],
            zr_sem.at[chunk],
            {"section": (s + sections - 1) % sections},
        )

    def z_slot(k):
        chunk = k - 2 * (sections - 1 - s)

        @pl.when((chunk >= 0) & (chunk < CHUNKS))
        def _():
            @pl.when(s < sections - 1)
            def _():
                z_copy(chunk).wait_recv()

            @pl.when(s == sections - 1)
            def _():
                zrecv[chunk] = jnp.zeros((tok, cw), BF16)

            for h in range(cw // 128):
                lanes = slice(h * 128, (h + 1) * 128)
                term = inv_v[...] * scaled[chunk, :, lanes] - xv[chunk, :, lanes].astype(F32) * coef_v[...]
                term = term + zrecv[chunk, :, lanes].astype(F32)
                zsend[chunk, :, lanes] = term.astype(BF16)
                og[chunk, :, lanes] = (tv[chunk, :, lanes].astype(F32) + term).astype(BF16)

            @pl.when(s > 0)
            def _():
                z_copy(chunk).start()

    ee[...] = jnp.zeros((BLOCK, BLOCK), F32)

    def n_forward(k, core):
        dx = k + k // 2 - 2 * (k // 3)
        index = at(dx, 0, core)
        return remote(
            n_slot(index), n_slot(index), nf_sem.at[2 * k + core], nr_sem.at[index], dp(at(0, 1, 1))
        )

    def n_home(k, core):
        dx = k % 4 + (k % 4) // 2 - 2 * ((k % 4) // 3)
        index = at(dx, k // 4, core)
        return remote(
            n_slot(index), n_slot(index), nd_sem.at[2 * k + core], nr_sem.at[index], dp(at(0, 0, 0))
        )

    @pl.when(feature_core)
    def _():
        def step(k, carry):
            for core in (1, 0):
                if core == 0:
                    n_home(k, core).wait_recv()
                else:

                    @pl.when(k > 0)
                    def _():
                        n_home(k, core).wait_recv()

                @pl.when(k < 4)
                def _():
                    n_forward(k % 4, core).start()

                n_home(k, core).start()
            dx = k % 4 + (k % 4) // 2 - 2 * ((k % 4) // 3)
            index = at(dx, k // 4, 0)
            rows = nbuf[pl.ds(pl.multiple_of(index * tok, 2 * tok), 2 * tok), :]
            ee[...] = ee[...] + dot_tn(rows, rows)

            @pl.when(k == 1)
            def _():
                term_ready()

            z_slot(k - 1)

            return carry

        lax.fori_loop(0, 8, step, 0)
        limit = sweeps[0, 0, owner[0, 0, x]].astype(F32)
        lim[...] = jnp.full((8, BLOCK), limit, F32)

    def c_place(k):
        high = (k + 6) // 8
        m = (k - 2) * high
        dx = high * (1 + 2 * (m % 3) - 3 * ((m % 3) // 2))
        dy = high * (m // 3) + (1 - high) * k
        return dx, dy

    def c_forward(core, k):
        index = at(0, 1, core)
        dx = (1, 3, 2)[k]
        return remote(
            c_slot(index), c_slot(index), cs_sem.at[5 + 3 * core + k], cr_sem.at[index], dp(at(dx, 0, 0))
        )

    def c_arrived(index):
        return remote(c_slot(index), c_slot(index), cs_sem.at[0], cr_sem.at[index], dp(at(1, 0, 0)))

    @pl.when(value_core)
    def _():
        def step(k, carry):
            dx, dy = c_place(k)
            for core in (0, 1):
                if core == 1:
                    c_arrived(at(dx, dy, core)).wait_recv()
                else:

                    @pl.when(k > 0)
                    def _():
                        c_arrived(at(dx, dy, core)).wait_recv()

                @pl.when(k == 1)
                def _():
                    for q in range(3):
                        c_forward(core, q).start()

            rows = cbuf[pl.ds(pl.multiple_of(at(dx, dy, 0) * tok, 2 * tok), 2 * tok), :]
            ee[...] = ee[...] + dot_tn(rows, rows)

            @pl.when(k == 6)
            def _():
                term_ready()

            z_slot(k - 6)

            return carry

        lax.fori_loop(0, 8, step, 0)
        other = sqr[8:9, :]
        own = jnp.full((1, 128), own_limit, F32)
        limit = jnp.where(y == t, own, other)
        for h in range(BLOCK // 128):
            lim[:, h * 128 : (h + 1) * 128] = jnp.broadcast_to(limit, (8, 128))

    diagonal = lax.broadcasted_iota(jnp.int32, (BLOCK, BLOCK), 0) == lax.broadcasted_iota(
        jnp.int32, (BLOCK, BLOCK), 1
    )
    matrix = ee[...] / tokens + jnp.where(diagonal, DAMPING, 0.0)
    norm = lax.rsqrt(jnp.sum(jnp.sum(matrix * matrix, axis=0, keepdims=True), axis=1, keepdims=True))
    ee[...] = matrix * norm
    xx[...] = jnp.where(diagonal, 1.0, 0.0) * norm

    def sweep(k, carry):
        eb[...] = ee[...].astype(BF16)

        @pl.when(k > 0)
        def _():
            old = xx[...]
            new = 2.0 * old - dot_nn(old.astype(BF16), eb[...])
            xx[...] = jnp.where(lim[0:1, :] > k.astype(F32), new, old)

        @pl.when(k == 0)
        def _():
            xx[...] = 2.0 * xx[...] - ee[...] * norm

        @pl.when(k < ITERS - 1)
        def _():
            e = ee[...]
            ee[...] = 2.0 * e - dot_nn(eb[...], eb[...])

        @pl.when(k % 2 == 1)
        def _():
            z_slot(2 + 5 * c + (k - 1) // 2)

        return carry

    lax.fori_loop(0, ITERS, sweep, 0)
    eb[...] = xx[...].astype(BF16)

    v_copy = remote(eb, vb, gv_s.at[0], gv_r.at[0], dp(at(0, 0, 1)))
    g_copy = remote(gb, gb, gv_s.at[1], gv_r.at[1], dp(at(0, 0, 1)))

    @pl.when(value_core)
    def _():
        v_copy.start()
        xx[...] = jnp.zeros((BLOCK, BLOCK), F32)

        def step(k, carry):
            dx = k % 4 + (k % 4) // 2 - 2 * ((k % 4) // 3)
            for core in (1, 0):
                n_home(k, core).wait_recv()
            rows = pl.ds(pl.multiple_of(at(dx, k // 4, 0) * tok, 2 * tok), 2 * tok)
            xx[...] = xx[...] + dot_tn(nbuf[rows, :], cbuf[rows, :])

            @pl.when(k % 3 == 1)
            def _():
                z_slot(5 + (k - 1) // 3)

            return carry

        lax.fori_loop(0, 8, step, 0)
        gb[...] = xx[...].astype(BF16)
        g_copy.start()

        def more(k, carry):
            z_slot(k)
            return carry

        lax.fori_loop(8, 11, more, 0)

    rows_q = BLOCK // 4

    def piece(dx, dy, q):
        return (((x + dx) % NX) * 2 + (y + dy) % 2) * 4 + q

    def to(dx, dy, q, n, device):
        index = piece(dx, dy, q)
        return remote(pv.at[index], pv.at[index], as_sem.at[n], ar_sem.at[index], dp(device))

    def arrived(dx, dy, q):
        return to(dx, dy, q, 0, at(0, 0, 1 - c))

    def run(events, my_core):
        started = []
        n = 0
        for dx, dy, q, arrives, goes in events:
            if arrives:
                arrived(dx, dy, q).wait_recv()
            for where in goes:
                copy = to(dx, dy, where[3] if len(where) > 3 else q, n, at(*where[:3]))
                copy.start()
                started.append(copy)
                n += 1
            yield
        for dx, dy, q in [
            (dx, dy, q)
            for dy in range(2)
            for dx in (0, 1, 3, 2)
            for q in ((2, 3) if my_core == 1 else (0, 1))
            if my_core == 0 or (dx, dy) != (0, 0)
        ]:
            arrived(dx, dy, q).wait_recv()
        for copy in started:
            copy.wait_send()

    @pl.when(feature_core)
    def _():
        right, left, up, across = (1, 0, 1), (3, 0, 1), (0, 1, 1), (0, 0, 0)
        g_copy.wait_recv()
        v_copy.wait_recv()
        events = [
            (0, 0, 0, False, (right, up, across)),
            (0, 0, 2, False, ((0, 1, 0), across)),
            (0, 0, 1, False, (left, left + (0,), right, up, across)),
            (0, 0, 3, False, ((0, 1, 0), across)),
        ]
        events += [
            (3, 0, 0, True, (right, up, across)),
            (1, 0, 1, True, (left, up, across)),
            (0, 1, 0, True, (across,)),
            (3, 0, 1, True, (up, across)),
            (1, 0, 0, True, (up, across)),
            (0, 1, 1, True, (across,)),
            (2, 0, 0, True, (up, across)),
            (2, 0, 1, True, (up, across)),
            (3, 1, 0, True, (across,)),
            (1, 1, 1, True, (across,)),
            (3, 1, 1, True, (across,)),
            (1, 1, 0, True, (across,)),
            (2, 1, 0, True, (across,)),
            (2, 1, 1, True, (across,)),
        ]
        steps = run(events, 1)
        for q in (0, 2, 1, 3):
            rows = slice(q * rows_q, (q + 1) * rows_q)
            first = dot_nn(eb[rows, :], gb[...]).astype(BF16)
            pv[piece(0, 0, q)] = dot_nn(first, vb[...]).astype(BF16)
            next(steps)
        z_slot(10)
        k = 11
        for number in range(len(events) - 4):
            next(steps)
            if number not in (0, 4, 8):
                z_slot(k)
                k += 1
        for _ in steps:
            pass

    @pl.when(value_core)
    def _():
        right, left, across = (1, 0, 0), (3, 0, 0), (0, 0, 1)
        events = [
            (0, 0, 2, True, (right,)),
            (0, 1, 2, True, (right, across)),
            (0, 0, 3, True, (left, left + (2,), right)),
            (0, 1, 3, True, (left, left + (2,), right, across)),
            (3, 0, 2, True, (right, across)),
            (1, 0, 3, True, (left, across)),
            (3, 1, 2, True, (right, across)),
            (1, 1, 3, True, (left, across)),
            (3, 0, 3, True, (across,)),
            (1, 0, 2, True, (across,)),
            (3, 1, 3, True, (across,)),
            (1, 1, 2, True, (across,)),
            (2, 0, 2, True, (across,)),
            (2, 0, 3, True, (across,)),
            (2, 1, 2, True, (across,)),
            (2, 1, 3, True, (across,)),
        ]
        steps = run(events, 0)
        k = 11
        for number in range(len(events)):
            next(steps)
            if number not in (0, 1, 4, 8, 12):
                z_slot(k)
                k += 1
        for _ in steps:
            pass

    squares_copy.wait_send()
    inner_copy.wait_send()
    for k in range(4):
        c_send(k).wait_send()
    for k in range(3):
        n_send(k).wait_send()

    @pl.when(feature_core)
    def _():
        c_home.wait_send()

        def ended(k, carry):
            for core in (1, 0):
                n_home(k, core).wait_send()

                @pl.when(k < 4)
                def _():
                    n_forward(k % 4, core).wait_send()

            return carry

        lax.fori_loop(0, 8, ended, 0)

    @pl.when(value_core)
    def _():
        n_send(3).wait_send()
        for core in range(2):
            for k in range(3):
                c_forward(core, k).wait_send()
        v_copy.wait_send()
        g_copy.wait_send()

    def chain_ended(chunk, carry):
        @pl.when(s > 0)
        def _():
            z_copy(chunk).wait_send()

        return carry

    lax.fori_loop(0, CHUNKS, chain_ended, 0)


def lay_out(chunks, pieces, grad_out, pre_out, grad_sem, pre_sem):
    copies = []
    cw = chunks.shape[2]
    rows = pieces.shape[1]
    for n in range(32):
        i, j, q = n // 8, (n // 4) % 2, n % 4
        out = pre_out.at[0, pl.ds(i * BLOCK + q * rows, rows), pl.ds(j * BLOCK, BLOCK)]
        copies.append(pltpu.make_async_copy(pieces.at[n], out, pre_sem.at[n]))
    for k in range(CHUNKS):
        out = grad_out.at[0, :, pl.ds(k * cw, cw)]
        copies.append(pltpu.make_async_copy(chunks.at[k], out, grad_sem.at[k]))
    for copy in copies:
        copy.start()
    for copy in copies:
        copy.wait()


def on_device(sections, tokens, activations, norm_gain, weights, cotangent, top_grad, owner_slot, sweeps):
    tok, half_width = activations.shape[1:]
    value_width = weights.shape[2]
    cw = half_width // CHUNKS
    vmem = functools.partial(pltpu.VMEM)
    dma = pltpu.SemaphoreType.DMA
    anywhere = pl.BlockSpec(memory_space=pl.ANY)
    hbm = pl.BlockSpec(memory_space=pltpu.HBM)
    smem = pl.BlockSpec(memory_space=pltpu.SMEM)
    chunks, pieces = pl.pallas_call(
        functools.partial(kernel, sections, tokens),
        out_shape=(
            pltpu.VMEM((CHUNKS, tok, cw), BF16),
            pltpu.VMEM((32, BLOCK // 4, BLOCK), BF16),
        ),
        in_specs=[
            smem,
            smem,
            hbm,
            pl.BlockSpec(memory_space=pltpu.VMEM),
            hbm,
            hbm,
            hbm,
        ],
        out_specs=(pl.BlockSpec(memory_space=pltpu.VMEM),) * 2,
        scratch_shapes=[
            vmem((CHUNKS, tok, cw), BF16),
            vmem((2, tok, BLOCK), BF16),
            vmem((half_width, value_width), BF16),
            vmem((CHUNKS, tok, cw), BF16),
            vmem((CHUNKS, tok, cw), F32),
            vmem((NF, tok, BLOCK), BF16),
            vmem((tok * 16, BLOCK), BF16),
            vmem((tok * 16, BLOCK), BF16),
            vmem((BLOCK, BLOCK), F32),
            vmem((BLOCK, BLOCK), F32),
            vmem((BLOCK, BLOCK), BF16),
            vmem((BLOCK, BLOCK), BF16),
            vmem((BLOCK, BLOCK), BF16),
            vmem((16, 128), F32),
            vmem((16, 128), F32),
            vmem((8, 128), F32),
            vmem((8, 128), F32),
            vmem((tok, 128), F32),
            vmem((tok, 128), F32),
            vmem((8, BLOCK), F32),
            vmem((CHUNKS, tok, cw), BF16),
            vmem((CHUNKS, tok, cw), BF16),
            dma((3 + 2 * CHUNKS,)),
            dma((11,)),
            dma((16,)),
            dma((4,)),
            dma((8,)),
            dma((16,)),
            dma((16,)),
            dma((2,)),
            dma((2,)),
            dma((CHUNKS,)),
            dma((CHUNKS,)),
            dma((2,)),
            dma((2,)),
            dma((40,)),
            dma((32,)),
        ],
        compiler_params=pltpu.CompilerParams(
            collective_id=0, has_side_effects=True, vmem_limit_bytes=60000 * 1024
        ),
        name="kfac",
    )(owner_slot, sweeps, activations, norm_gain, weights, cotangent, top_grad)
    return pl.pallas_call(
        lay_out,
        out_shape=(
            jax.ShapeDtypeStruct((1, tok, half_width), BF16),
            jax.ShapeDtypeStruct((1, half_width, value_width), BF16),
        ),
        in_specs=[anywhere, anywhere],
        out_specs=(anywhere, anywhere),
        scratch_shapes=[dma((CHUNKS,)), dma((32,))],
        compiler_params=pltpu.CompilerParams(vmem_limit_bytes=1 << 20),
        name="lay_out",
    )(chunks, pieces)


def solution(mesh):
    sections = mesh.shape["section"]
    placed = (
        P("section", "dp", "tensor"),
        P("section", "tensor"),
        P("section", "tensor", None),
        P("section", "dp", None),
        P("dp", "tensor"),
        P("section", "tensor", None),
        P("section", "tensor", None),
    )

    def step(activations, *rest):
        return on_device(sections, activations.shape[1] * 16, activations, *rest)

    return jax.shard_map(
        step,
        mesh=mesh,
        in_specs=placed,
        out_specs=(P("section", "dp", "tensor"), P("section", "tensor", None)),
        check_vma=False,
    )
```

```python
import functools

import jax
import jax.numpy as jnp
from jax import lax
from jax.experimental import pallas as pl
from jax.experimental.pallas import tpu as pltpu
from jax.sharding import PartitionSpec as P

BLOCK = 512
ITERS = 6
EPSILON = 1e-05
DAMPING = 0.05
NX = 4
NF = 4
CHUNKS = 8
LINKS = 16
MESH = pl.DeviceIdType.MESH
F32 = jnp.float32
BF16 = jnp.bfloat16


def remote(src, dst, send, recv, device):
    return pltpu.make_async_remote_copy(
        src_ref=src,
        dst_ref=dst,
        send_sem=send,
        recv_sem=recv,
        device_id=device,
        device_id_type=MESH,
    )


def as_row(partial):
    return jnp.broadcast_to(jnp.sum(partial.T, axis=0, keepdims=True), (8, partial.shape[0]))


def as_column(row):
    return jnp.broadcast_to(row, (row.shape[1], row.shape[1])).T


def dot_tn(a, b):
    return lax.dot_general(a, b, (((0,), (0,)), ((), ())), preferred_element_type=F32)


def dot_nt(a, b):
    return lax.dot_general(a, b, (((1,), (1,)), ((), ())), preferred_element_type=F32)


def dot_nn(a, b):
    return lax.dot_general(a, b, (((1,), (0,)), ((), ())), preferred_element_type=F32)


def kernel(
    sections,
    tokens,
    owner,
    sweeps,
    act,
    gain,
    weights,
    cot,
    top,
    og,
    pv,
    xv,
    cv,
    wv,
    tv,
    scaled,
    nbuf,
    nn,
    cbuf,
    gacc,
    fsq,
    ee,
    xx,
    eb,
    gb,
    vb,
    lb,
    sqs,
    sqr,
    ins,
    inr,
    inv_v,
    coef_v,
    lim,
    zsend,
    zrecv,
    relay,
    load_sem,
    cs_sem,
    cr_sem,
    cb_sem,
    fs_sem,
    fr_sem,
    ns_sem,
    nf_sem,
    nr_sem,
    rs_sem,
    rr_sem,
    small_s,
    small_r,
    zs_sem,
    zr_sem,
    gv_s,
    gv_r,
    as_sem,
    ar_sem,
):
    s = lax.axis_index("section")
    r = lax.axis_index("dp")
    t = lax.axis_index("tensor")
    x = r // 4
    y = (r // 2) % 2
    c = r % 2
    tok = xv.shape[1]
    cw = scaled.shape[2]
    full = NF * BLOCK * 2

    def at(dx, dy, core):
        return (((x + dx) % NX) * 2 + (y + dy) % 2) * 2 + core

    def dp(index):
        return {"dp": index}

    loads = []
    for j in range(2):
        loads.append(
            pltpu.make_async_copy(
                cot.at[0, :, pl.ds(j * BLOCK, BLOCK)], cv.at[j], load_sem.at[j]
            )
        )
    for k in range(NF):
        loads.append(
            pltpu.make_async_copy(
                act.at[0, :, pl.ds(k * BLOCK, BLOCK)], xv.at[k], load_sem.at[2 + k]
            )
        )
    loads.append(pltpu.make_async_copy(weights.at[0], wv, load_sem.at[2 + NF]))
    for k in range(NF):
        loads.append(
            pltpu.make_async_copy(
                top.at[:, pl.ds(k * BLOCK, BLOCK)], tv.at[k], load_sem.at[3 + NF + k]
            )
        )
    for load in loads:
        load.start()

    barrier = pltpu.get_barrier_semaphore()
    for k in range(1, 32):
        other = (16 * t + r + k) % 32
        pl.semaphore_signal(
            barrier, inc=1, device_id={"dp": other % 16, "tensor": other // 16}, device_id_type=MESH
        )

    @pl.when(s < sections - 1)
    def _():
        pl.semaphore_signal(barrier, inc=1, device_id={"section": s + 1}, device_id_type=MESH)

    for k in range(NF):
        loads[2 + k].wait()

    def square_step(k, total):
        v = xv[k].astype(F32)
        v = v * v
        for h in range(BLOCK // 128):
            total = total + v[:, h * 128 : (h + 1) * 128]
        return total

    squares = lax.fori_loop(0, NF, square_step, jnp.zeros((tok, 128), F32))
    own_limit = sweeps[0, 0, owner[0, 0, NF]].astype(F32)
    sqs[0:8, :] = as_row(squares)
    sqs[8:16, :] = jnp.full((8, 128), own_limit, F32)
    loads[0].wait()
    loads[1].wait()

    @pl.when(s > 0)
    def _():
        pl.semaphore_wait(barrier, 32)

    @pl.when(s == 0)
    def _():
        pl.semaphore_wait(barrier, 31)

    partner = {"tensor": 1 - t}
    squares_copy = remote(sqs, sqr, small_s.at[0], small_r.at[0], partner)
    squares_copy.start()

    value_core = c == 0
    feature_core = c == 1

    def c_slot(index):
        return cbuf.at[pl.ds(pl.multiple_of(index * tok, tok), tok), :]

    def n_slot(index):
        return nbuf.at[pl.ds(pl.multiple_of(index * tok, tok), tok), :]

    def c_send(k):
        if k == 0:
            return remote(cv.at[1 - y], c_slot(r), cs_sem.at[0], cr_sem.at[r], dp(at(0, 1, 0)))
        dx = (None, 1, 3)[k]
        return remote(cv.at[y], c_slot(r), cs_sem.at[k], cr_sem.at[r], dp(at(dx, 0, 0)))

    c_home = remote(cv.at[y], c_slot(r), cs_sem.at[3], cr_sem.at[r], dp(at(0, 0, 0)))
    def f_send(k):
        dx, dy, half = k % 4, (k // 4) % 2, (t + k // 8) % 2
        own = 16 * t + r
        return remote(
            sqs.at[0:8, :], fsq.at[own], fs_sem.at[k], fr_sem.at[own], {"dp": at(dx, dy, 1), "tensor": half}
        )

    def n_send(k):
        if k == 0:
            return remote(xv.at[x], n_slot(r), ns_sem.at[k], nr_sem.at[r], dp(at(0, 1, 1)))
        if k == 3:
            return remote(
                xv.at[(x + 2) % NX], relay.at[c], ns_sem.at[k], rr_sem.at[c], dp(at(1 + 2 * c, 0, 1))
            )
        dx = (None, 1, 3, None, 0)[k]
        return remote(xv.at[(x + dx) % NX], n_slot(r), ns_sem.at[k], nr_sem.at[r], dp(at(dx, 0, 1)))

    for k in range(1, 16):
        f_send(k).start()

    @pl.when(value_core)
    def _():
        f_send(0).start()
        n_send(4).start()

    @pl.when(feature_core)
    def _():
        c_home.start()

    c_send(0).start()
    for k in range(1, 3):
        n_send(k).start()
    for k in range(1, 3):
        c_send(k).start()
    n_send(3).start()

    @pl.when(value_core)
    def _():
        c_slot(r)[...] = cv[y]

    @pl.when(feature_core)
    def _():
        c_slot(r)[...] = cv[y]
        n_slot(r)[...] = xv[x]
        fsq[16 * t + r] = sqs[0:8, :]

    loads[2 + NF].wait()

    def x_lanes(k, h):
        per = BLOCK // cw
        lane = pl.multiple_of((k % per) * cw + h * 128, 128)
        return xv[k // per, :, pl.ds(lane, 128)].astype(F32)

    def upstream_step(k, total):
        rows = pl.ds(pl.multiple_of(k * cw, cw), cw)
        up = dot_nt(cv[0], wv[rows, pl.ds(0, BLOCK)]) + dot_nt(cv[1], wv[rows, pl.ds(BLOCK, BLOCK)])
        up = up * gain[0:1, pl.ds(pl.multiple_of(k * cw, cw), cw)]
        scaled[k] = up
        for h in range(cw // 128):
            total = total + up[:, h * 128 : (h + 1) * 128] * x_lanes(k, h)
        return total

    inner = lax.fori_loop(0, CHUNKS, upstream_step, jnp.zeros((tok, 128), F32))
    ins[...] = as_row(inner)
    inner_copy = remote(ins, inr, small_s.at[1], small_r.at[1], partner)
    inner_copy.start()
    n_send(0).start()

    def term_ready():
        squares_copy.wait_recv()
        inner_copy.wait_recv()
        row = lax.rsqrt((sqs[0:1, :] + sqr[0:1, :]) / full + EPSILON)
        inv_v[...] = as_column(row)
        coef_v[...] = as_column(row * row * row * (ins[0:1, :] + inr[0:1, :]) / full)
        for k in range(NF):
            loads[3 + NF + k].wait()

    def z_copy(chunk):
        return remote(
            zsend.at[chunk],
            zrecv.at[chunk],
            zs_sem.at[chunk],
            zr_sem.at[chunk],
            {"section": (s + sections - 1) % sections},
        )

    def z_step(chunk):
        @pl.when(s < sections - 1)
        def _():
            z_copy(chunk).wait_recv()

        @pl.when(s == sections - 1)
        def _():
            zrecv[chunk] = jnp.zeros((tok, 128), BF16)

        up = scaled[chunk * 128 // cw, :, pl.ds(pl.multiple_of(chunk * 128 % cw, 128), 128)]
        block = chunk * 128 // BLOCK
        lanes = pl.ds(pl.multiple_of(chunk * 128 % BLOCK, 128), 128)
        term = inv_v[...] * up - xv[block, :, lanes].astype(F32) * coef_v[...]
        term = term + zrecv[chunk].astype(F32)
        zsend[chunk] = term.astype(BF16)
        columns = pl.ds(pl.multiple_of(chunk * 128, 128), 128)
        og[:, columns] = (tv[block, :, lanes].astype(F32) + term).astype(BF16)

        @pl.when(s > 0)
        def _():
            z_copy(chunk).start()

    def z_count(when):
        come = (2 * (when - 140 - 33 * (sections - 1 - s)) + 3000) // 15 - 199
        come = come + LINKS * (s // (sections - 1)) * (when // 110)
        return jnp.minimum(jnp.maximum(come, 0), LINKS) * ((s + sections - 1) // sections)

    def z_point(last, now):
        def step(chunk, carry):
            z_step(chunk)
            return carry

        lax.fori_loop(z_count(last), z_count(now), step, 0)

    def z_end():
        @pl.when(s == 0)
        def _():
            def step(chunk, carry):
                z_step(chunk)
                return carry

            lax.fori_loop(0, LINKS, step, 0)

    ee[...] = jnp.zeros((BLOCK, BLOCK), F32)

    def place(k):
        high = k // 6
        return (1 - high) * (k % 3 + (k % 3) // 2) + 2 * high, (1 - high) * (k // 3) + high * (k % 2)

    def n_forward(k, core):
        index = at((0, 1, 3, 2)[k], 0, core)
        return remote(
            n_slot(index), n_slot(index), nf_sem.at[2 * k + core], nr_sem.at[index], dp(at(0, 1, 1))
        )

    def n_arrived(index):
        return remote(n_slot(index), n_slot(index), nf_sem.at[0], nr_sem.at[index], dp(at(0, 1, 1)))

    def f_arrived(index):
        return remote(fsq.at[index], fsq.at[index], fs_sem.at[0], fr_sem.at[index], dp(at(0, 1, 1)))

    def c_arrived(index):
        return remote(c_slot(index), c_slot(index), cs_sem.at[0], cr_sem.at[index], dp(at(1, 0, 0)))

    def c_back(index):
        return remote(c_slot(index), c_slot(index), cb_sem.at[index], cr_sem.at[index], dp(at(0, 0, 1)))

    def norm_slot(index):
        total = fsq[index][0:1, :] + fsq[16 + index][0:1, :]
        inverse = as_column(lax.rsqrt(total / full + EPSILON))
        rows = pl.ds(pl.multiple_of(index * tok, tok), tok)
        for h in range(BLOCK // 128):
            lanes = slice(h * 128, (h + 1) * 128)
            row = gain[0:1, pl.ds(pl.multiple_of(x * BLOCK + h * 128, 128), 128)]
            nn[rows, lanes] = (nbuf[rows, lanes].astype(F32) * inverse * row).astype(BF16)

    def n_relay(side):
        dx = (3, 1)[side]
        return remote(
            relay.at[side],
            n_slot(at(dx, 0, side)),
            rs_sem.at[side],
            nr_sem.at[at(dx, 0, side)],
            dp(at((1, 3)[side], 0, 1)),
        )

    def n_relayed(side):
        return remote(relay.at[side], relay.at[side], rs_sem.at[side], rr_sem.at[side], dp(at(1, 0, 1)))

    def pair(k):
        dx, dy = place(k)
        return pl.ds(pl.multiple_of(at(dx, dy, 0) * tok, 2 * tok), 2 * tok)

    def add_grad(k):
        dx, dy = place(k)

        @pl.when(k > 0)
        def _():
            c_arrived(at(dx, dy, 1)).wait_recv()

        c_arrived(at(dx, dy, 0)).wait_recv()
        gacc[...] = gacc[...] + dot_tn(nn[pair(k), :], cbuf[pair(k), :])

    @pl.when(feature_core)
    def _():
        gacc[...] = jnp.zeros((BLOCK, BLOCK), F32)

        def pass_on(k):
            for core in (1, 0):
                n_arrived(at((0, 1, 3, 2)[k], 0, core)).wait_recv()
                n_forward(k, core).start()

        def step_time(k):
            late = (k + 6) // 8
            return late * (172 + 13 * k) + (1 - late) * (128 + 22 * k)

        def step(k, carry):
            dx, dy = place(k)

            @pl.when(k == 1)
            def _():
                pass_on(1)
                pass_on(2)

            @pl.when(k == 2)
            def _():
                for side in range(2):
                    n_relayed(side).wait_recv()
                    n_relay(side).start()

            @pl.when(k == 4)
            def _():
                pass_on(3)

            @pl.when(((k > 2) & (k < 6)) | (k == 7))
            def _():
                n_arrived(at(dx, dy, 1)).wait_recv()

            @pl.when((k == 0) | ((k > 2) & (k < 6)) | (k == 7))
            def _():
                n_arrived(at(dx, dy, 0)).wait_recv()

            for core in (1, 0):
                index = at(dx, dy, core)
                f_arrived(index + 16 * (1 - t)).wait_recv()
                if core == 0:
                    f_arrived(index + 16 * t).wait_recv()
                else:

                    @pl.when(k > 0)
                    def _():
                        f_arrived(index + 16 * t).wait_recv()

                norm_slot(index)
            ee[...] = ee[...] + dot_tn(nn[pair(k), :], nn[pair(k), :])

            @pl.when(k == 0)
            def _():
                term_ready()

            @pl.when(k > 0)
            def _():
                add_grad(k - 1)

            z_point(step_time(k - 1), step_time(k))
            return carry

        lax.fori_loop(0, 8, step, 0)
        limit = sweeps[0, 0, owner[0, 0, x]].astype(F32)
        lim[...] = jnp.full((8, BLOCK), limit, F32)

    def c_place(k):
        low, high = (7 - k) // 6, k // 6
        middle = 1 - low - high
        dx = middle * (1 + 2 * (k % 2)) + high * 2
        dy = (low + high) * (k % 2) + middle * (k // 2 - 1)
        return dx, dy

    def c_forward(dx, dy, core, to_right, n):
        index = at(dx, dy, core)
        return remote(
            c_slot(index),
            c_slot(index),
            cs_sem.at[n],
            cr_sem.at[index],
            dp(at(1 if to_right else 3, 0, 0)),
        )

    c_forwards = {
        1: [(0, 1, core, way, 4 + 2 * core + way) for core in range(2) for way in range(2)],
        2: [(1, 0, 1, 0, 8)],
        3: [(3, 0, 0, 1, 9)],
        4: [(1, 1, 1, 0, 10)],
        5: [(3, 1, 0, 1, 11)],
    }

    @pl.when(value_core)
    def _():
        def step(k, carry):
            dx, dy = c_place(k)
            for core in (0, 1):
                if core == 1:
                    c_arrived(at(dx, dy, core)).wait_recv()
                else:

                    @pl.when(k > 0)
                    def _():
                        c_arrived(at(dx, dy, core)).wait_recv()

                if core == 0:
                    c_back(at(dx, dy, core)).start()
                else:

                    @pl.when(k > 0)
                    def _():
                        c_back(at(dx, dy, core)).start()

            for number, forwards in c_forwards.items():

                @pl.when(k == number)
                def _():
                    for forward in forwards:
                        c_forward(*forward).start()

            rows = cbuf[pl.ds(pl.multiple_of(at(dx, dy, 0) * tok, 2 * tok), 2 * tok), :]
            ee[...] = ee[...] + dot_tn(rows, rows)

            @pl.when(k == 1)
            def _():
                term_ready()

            z_point(89 + 20 * k, 109 + 20 * k)

            return carry

        lax.fori_loop(0, 8, step, 0)
        other = sqr[8:9, :]
        own = jnp.full((1, 128), own_limit, F32)
        limit = jnp.where(y == t, own, other)
        for h in range(BLOCK // 128):
            lim[:, h * 128 : (h + 1) * 128] = jnp.broadcast_to(limit, (8, 128))

    diagonal = lax.broadcasted_iota(jnp.int32, (BLOCK, BLOCK), 0) == lax.broadcasted_iota(
        jnp.int32, (BLOCK, BLOCK), 1
    )
    matrix = ee[...] / tokens + jnp.where(diagonal, DAMPING, 0.0)
    norm = lax.rsqrt(jnp.sum(jnp.sum(matrix * matrix, axis=0, keepdims=True), axis=1, keepdims=True))
    ee[...] = matrix * norm
    xx[...] = jnp.where(diagonal, 1.0, 0.0) * norm

    def sweep(k, carry):
        eb[...] = ee[...].astype(BF16)

        @pl.when(k > 0)
        def _():
            old = xx[...]
            new = 2.0 * old - dot_nn(old.astype(BF16), eb[...])
            xx[...] = jnp.where(lim[0:1, :] > k.astype(F32), new, old)

        @pl.when(k == 0)
        def _():
            xx[...] = 2.0 * xx[...] - ee[...] * norm

        @pl.when(k < ITERS - 1)
        def _():
            e = ee[...]
            ee[...] = 2.0 * e - dot_nn(eb[...], eb[...])

        @pl.when((c == 1) & (k == 2))
        def _():
            add_grad(jnp.int32(7))
            gb[...] = gacc[...].astype(BF16)

        before = (10 + 14 * c) * (1 - (k + 5) // 6)
        z_point(259 + 28 * c + 10 * k - before, 269 + 28 * c + 10 * k)

        return carry

    lax.fori_loop(0, ITERS, sweep, 0)
    eb[...] = xx[...].astype(BF16)

    v_copy = remote(eb, vb, gv_s.at[0], gv_r.at[0], dp(at(0, 0, 1)))

    @pl.when(value_core)
    def _():
        v_copy.start()

        z_point(319, 335)

    rows_q = BLOCK // 4

    def piece(dx, dy, q):
        return (((x + dx) % NX) * 2 + (y + dy) % 2) * 4 + q

    def to(dx, dy, q, n, device):
        index = piece(dx, dy, q)
        return remote(pv.at[index], pv.at[index], as_sem.at[n], ar_sem.at[index], dp(device))

    def arrived(dx, dy, q):
        return to(dx, dy, q, 0, at(0, 0, 1 - c))

    def run(events, my_core):
        started = []
        n = 0
        for dx, dy, q, arrives, goes in events:
            if arrives:
                arrived(dx, dy, q).wait_recv()
            for where in goes:
                copy = to(dx, dy, where[3] if len(where) > 3 else q, n, at(*where[:3]))
                copy.start()
                started.append(copy)
                n += 1
            yield
        for dx, dy, q in [
            (dx, dy, q)
            for dy in range(2)
            for dx in (0, 1, 3, 2)
            for q in ((2, 3) if my_core == 1 else (0, 1))
            if my_core == 0 or (dx, dy) != (0, 0)
        ]:
            arrived(dx, dy, q).wait_recv()
        for copy in started:
            copy.wait_send()

    @pl.when(feature_core)
    def _():
        right, left, up, across = (1, 0, 1), (3, 0, 1), (0, 1, 1), (0, 0, 0)
        z_point(347, 350)
        lb[...] = dot_nn(eb[...], gb[...]).astype(BF16)
        v_copy.wait_recv()
        events = [
            (0, 0, 0, False, (right, up, across)),
            (0, 0, 2, False, ((0, 1, 0), across)),
            (0, 0, 1, False, (left, left + (0,), right, up, across)),
            (0, 0, 3, False, ((0, 1, 0), across)),
        ]
        events += [
            (3, 0, 0, True, (right, up, across)),
            (1, 0, 1, True, (left, up, across)),
            (0, 1, 0, True, (across,)),
            (3, 0, 1, True, (up, across)),
            (1, 0, 0, True, (up, across)),
            (0, 1, 1, True, (across,)),
            (2, 0, 0, True, (up, across)),
            (2, 0, 1, True, (up, across)),
            (3, 1, 0, True, (across,)),
            (1, 1, 1, True, (across,)),
            (3, 1, 1, True, (across,)),
            (1, 1, 0, True, (across,)),
            (2, 1, 0, True, (across,)),
            (2, 1, 1, True, (across,)),
        ]
        steps = run(events, 1)
        for q in (0, 2, 1, 3):
            rows = slice(q * rows_q, (q + 1) * rows_q)
            pv[piece(0, 0, q)] = dot_nn(lb[rows, :], vb[...]).astype(BF16)
            next(steps)
        z_point(350, 366)
        time = 366
        for number in range(len(events) - 4):
            next(steps)
            now = 376 + 9 * number if number < len(events) - 5 else 9000
            z_point(time, now)
            time = now
        z_end()
        for _ in steps:
            pass

    @pl.when(value_core)
    def _():
        right, left, across = (1, 0, 0), (3, 0, 0), (0, 0, 1)
        events = [
            (0, 0, 2, True, (right,)),
            (0, 1, 2, True, (right, across)),
            (0, 0, 3, True, (left, left + (2,), right)),
            (0, 1, 3, True, (left, left + (2,), right, across)),
            (3, 0, 2, True, (right, across)),
            (1, 0, 3, True, (left, across)),
            (3, 1, 2, True, (right, across)),
            (1, 1, 3, True, (left, across)),
            (3, 0, 3, True, (across,)),
            (1, 0, 2, True, (across,)),
            (3, 1, 3, True, (across,)),
            (1, 1, 2, True, (across,)),
            (2, 0, 2, True, (across,)),
            (2, 0, 3, True, (across,)),
            (2, 1, 2, True, (across,)),
            (2, 1, 3, True, (across,)),
        ]
        steps = run(events, 0)
        time = 335
        for number in range(len(events)):
            next(steps)
            now = 345 + 9 * number if number < len(events) - 1 else 9000
            z_point(time, now)
            time = now
        z_end()
        for _ in steps:
            pass

    squares_copy.wait_send()
    inner_copy.wait_send()
    for k in range(3):
        c_send(k).wait_send()
    for k in range(4):
        n_send(k).wait_send()
    for k in range(1, 16):
        f_send(k).wait_send()

    @pl.when(feature_core)
    def _():
        c_home.wait_send()
        for side in range(2):
            n_relay(side).wait_send()

        for k in range(1, 4):
            for core in range(2):
                n_forward(k, core).wait_send()

    @pl.when(value_core)
    def _():
        f_send(0).wait_send()
        n_send(4).wait_send()

        def ended(k, carry):
            dx, dy = place(k)
            c_back(at(dx, dy, 0)).wait_send()

            @pl.when(k > 0)
            def _():
                c_back(at(dx, dy, 1)).wait_send()

            return carry

        lax.fori_loop(0, 8, ended, 0)
        for forwards in c_forwards.values():
            for forward in forwards:
                c_forward(*forward).wait_send()
        v_copy.wait_send()

    def chain_ended(chunk, carry):
        @pl.when(s > 0)
        def _():
            z_copy(chunk).wait_send()

        return carry

    lax.fori_loop(0, LINKS, chain_ended, 0)


def lay_out(grad, pieces, grad_out, pre_out, grad_sem, pre_sem):
    copies = []
    rows = pieces.shape[1]
    for n in range(32):
        i, j, q = n // 8, (n // 4) % 2, n % 4
        out = pre_out.at[0, pl.ds(i * BLOCK + q * rows, rows), pl.ds(j * BLOCK, BLOCK)]
        copies.append(pltpu.make_async_copy(pieces.at[n], out, pre_sem.at[n]))
    copies.append(pltpu.make_async_copy(grad, grad_out.at[0], grad_sem.at[0]))
    for copy in copies:
        copy.start()
    for copy in copies:
        copy.wait()


def on_device(sections, tokens, activations, norm_gain, weights, cotangent, top_grad, owner_slot, sweeps):
    tok, half_width = activations.shape[1:]
    value_width = weights.shape[2]
    cw = half_width // CHUNKS
    vmem = functools.partial(pltpu.VMEM)
    dma = pltpu.SemaphoreType.DMA
    anywhere = pl.BlockSpec(memory_space=pl.ANY)
    hbm = pl.BlockSpec(memory_space=pltpu.HBM)
    smem = pl.BlockSpec(memory_space=pltpu.SMEM)
    grad, pieces = pl.pallas_call(
        functools.partial(kernel, sections, tokens),
        out_shape=(
            pltpu.VMEM((tok, half_width), BF16),
            pltpu.VMEM((32, BLOCK // 4, BLOCK), BF16),
        ),
        in_specs=[
            smem,
            smem,
            hbm,
            pl.BlockSpec(memory_space=pltpu.VMEM),
            hbm,
            hbm,
            hbm,
        ],
        out_specs=(pl.BlockSpec(memory_space=pltpu.VMEM),) * 2,
        scratch_shapes=[
            vmem((NF, tok, BLOCK), BF16),
            vmem((2, tok, BLOCK), BF16),
            vmem((half_width, value_width), BF16),
            vmem((NF, tok, BLOCK), BF16),
            vmem((CHUNKS, tok, cw), F32),
            vmem((tok * 16, BLOCK), BF16),
            vmem((tok * 16, BLOCK), BF16),
            vmem((tok * 16, BLOCK), BF16),
            vmem((BLOCK, BLOCK), F32),
            vmem((32, 8, 128), F32),
            vmem((BLOCK, BLOCK), F32),
            vmem((BLOCK, BLOCK), F32),
            vmem((BLOCK, BLOCK), BF16),
            vmem((BLOCK, BLOCK), BF16),
            vmem((BLOCK, BLOCK), BF16),
            vmem((BLOCK, BLOCK), BF16),
            vmem((16, 128), F32),
            vmem((16, 128), F32),
            vmem((8, 128), F32),
            vmem((8, 128), F32),
            vmem((tok, 128), F32),
            vmem((tok, 128), F32),
            vmem((8, BLOCK), F32),
            vmem((LINKS, tok, 128), BF16),
            vmem((LINKS, tok, 128), BF16),
            vmem((2, tok, BLOCK), BF16),
            dma((3 + 2 * NF,)),
            dma((12,)),
            dma((16,)),
            dma((16,)),
            dma((16,)),
            dma((32,)),
            dma((5,)),
            dma((8,)),
            dma((16,)),
            dma((2,)),
            dma((2,)),
            dma((2,)),
            dma((2,)),
            dma((LINKS,)),
            dma((LINKS,)),
            dma((1,)),
            dma((1,)),
            dma((40,)),
            dma((32,)),
        ],
        compiler_params=pltpu.CompilerParams(
            collective_id=0, has_side_effects=True, vmem_limit_bytes=60000 * 1024
        ),
        name="kfac",
    )(owner_slot, sweeps, activations, norm_gain, weights, cotangent, top_grad)
    return pl.pallas_call(
        lay_out,
        out_shape=(
            jax.ShapeDtypeStruct((1, tok, half_width), BF16),
            jax.ShapeDtypeStruct((1, half_width, value_width), BF16),
        ),
        in_specs=[anywhere, anywhere],
        out_specs=(anywhere, anywhere),
        scratch_shapes=[dma((1,)), dma((32,))],
        compiler_params=pltpu.CompilerParams(vmem_limit_bytes=1 << 20),
        name="lay_out",
    )(grad, pieces)


def solution(mesh):
    sections = mesh.shape["section"]
    placed = (
        P("section", "dp", "tensor"),
        P("section", "tensor"),
        P("section", "tensor", None),
        P("section", "dp", None),
        P("dp", "tensor"),
        P("section", "tensor", None),
        P("section", "tensor", None),
    )

    def step(activations, *rest):
        return on_device(sections, activations.shape[1] * 16, activations, *rest)

    return jax.shard_map(
        step,
        mesh=mesh,
        in_specs=placed,
        out_specs=(P("section", "dp", "tensor"), P("section", "tensor", None)),
        check_vma=False,
    )
```

```python
import functools

import jax
import jax.numpy as jnp
from jax import lax
from jax.experimental import pallas as pl
from jax.experimental.pallas import tpu as pltpu
from jax.sharding import PartitionSpec as P

BLOCK = 512
ITERS = 6
EPSILON = 1e-05
DAMPING = 0.05
NX = 4
NF = 4
CHUNKS = 8
LINKS = 16
MESH = pl.DeviceIdType.MESH
F32 = jnp.float32
BF16 = jnp.bfloat16


def remote(src, dst, send, recv, device):
    return pltpu.make_async_remote_copy(
        src_ref=src,
        dst_ref=dst,
        send_sem=send,
        recv_sem=recv,
        device_id=device,
        device_id_type=MESH,
    )


def as_row(partial):
    return jnp.broadcast_to(jnp.sum(partial.T, axis=0, keepdims=True), (8, partial.shape[0]))


def as_column(row):
    return jnp.broadcast_to(row, (row.shape[1], row.shape[1])).T


def dot_tn(a, b):
    return lax.dot_general(a, b, (((0,), (0,)), ((), ())), preferred_element_type=F32)


def dot_nt(a, b):
    return lax.dot_general(a, b, (((1,), (1,)), ((), ())), preferred_element_type=F32)


def dot_nn(a, b):
    return lax.dot_general(a, b, (((1,), (0,)), ((), ())), preferred_element_type=F32)


def kernel(
    sections,
    tokens,
    owner,
    sweeps,
    act,
    gain,
    weights,
    cot,
    top,
    og,
    pv,
    xv,
    cv,
    wv,
    tv,
    scaled,
    nbuf,
    nn,
    cbuf,
    gacc,
    fsq,
    ee,
    xx,
    eb,
    gb,
    vb,
    lb,
    sqs,
    sqr,
    ins,
    inr,
    inv_v,
    coef_v,
    lim,
    zsend,
    zrecv,
    relay,
    load_sem,
    cs_sem,
    cr_sem,
    cb_sem,
    fs_sem,
    fr_sem,
    ns_sem,
    nf_sem,
    nr_sem,
    rs_sem,
    rr_sem,
    small_s,
    small_r,
    zs_sem,
    zr_sem,
    gv_s,
    gv_r,
    as_sem,
    ar_sem,
):
    s = lax.axis_index("section")
    r = lax.axis_index("dp")
    t = lax.axis_index("tensor")
    x = r // 4
    y = (r // 2) % 2
    c = r % 2
    tok = xv.shape[1]
    cw = scaled.shape[2]
    full = NF * BLOCK * 2

    def at(dx, dy, core):
        return (((x + dx) % NX) * 2 + (y + dy) % 2) * 2 + core

    def dp(index):
        return {"dp": index}

    loads = []
    for j in range(2):
        loads.append(
            pltpu.make_async_copy(
                cot.at[0, :, pl.ds(j * BLOCK, BLOCK)], cv.at[j], load_sem.at[j]
            )
        )
    for k in range(NF):
        loads.append(
            pltpu.make_async_copy(
                act.at[0, :, pl.ds(k * BLOCK, BLOCK)], xv.at[k], load_sem.at[2 + k]
            )
        )
    loads.append(pltpu.make_async_copy(weights.at[0], wv, load_sem.at[2 + NF]))
    for k in range(NF):
        loads.append(
            pltpu.make_async_copy(
                top.at[:, pl.ds(k * BLOCK, BLOCK)], tv.at[k], load_sem.at[3 + NF + k]
            )
        )
    for load in loads:
        load.start()

    barrier = pltpu.get_barrier_semaphore()
    for k in range(1, 32):
        other = (16 * t + r + k) % 32
        pl.semaphore_signal(
            barrier, inc=1, device_id={"dp": other % 16, "tensor": other // 16}, device_id_type=MESH
        )

    @pl.when(s < sections - 1)
    def _():
        pl.semaphore_signal(barrier, inc=1, device_id={"section": s + 1}, device_id_type=MESH)

    for k in range(NF):
        loads[2 + k].wait()

    def square_step(k, total):
        v = xv[k].astype(F32)
        v = v * v
        for h in range(BLOCK // 128):
            total = total + v[:, h * 128 : (h + 1) * 128]
        return total

    squares = lax.fori_loop(0, NF, square_step, jnp.zeros((tok, 128), F32))
    own_limit = sweeps[0, 0, owner[0, 0, NF]].astype(F32)
    sqs[0:8, :] = as_row(squares)
    sqs[8:16, :] = jnp.full((8, 128), own_limit, F32)
    loads[0].wait()
    loads[1].wait()

    @pl.when(s > 0)
    def _():
        pl.semaphore_wait(barrier, 32)

    @pl.when(s == 0)
    def _():
        pl.semaphore_wait(barrier, 31)

    partner = {"tensor": 1 - t}
    squares_copy = remote(sqs, sqr, small_s.at[0], small_r.at[0], partner)
    squares_copy.start()

    value_core = c == 0
    feature_core = c == 1

    def c_slot(index):
        return cbuf.at[pl.ds(pl.multiple_of(index * tok, tok), tok), :]

    def n_slot(index):
        return nbuf.at[pl.ds(pl.multiple_of(index * tok, tok), tok), :]

    def c_send(k):
        if k == 0:
            return remote(cv.at[1 - y], c_slot(r), cs_sem.at[0], cr_sem.at[r], dp(at(0, 1, 0)))
        dx = (None, 1, 3)[k]
        return remote(cv.at[y], c_slot(r), cs_sem.at[k], cr_sem.at[r], dp(at(dx, 0, 0)))

    c_home = remote(cv.at[y], c_slot(r), cs_sem.at[3], cr_sem.at[r], dp(at(0, 0, 0)))
    def f_send(k):
        dx, dy, half = k % 4, (k // 4) % 2, (t + k // 8) % 2
        own = 16 * t + r
        return remote(
            sqs.at[0:8, :], fsq.at[own], fs_sem.at[k], fr_sem.at[own], {"dp": at(dx, dy, 1), "tensor": half}
        )

    def n_send(k):
        if k == 0:
            return remote(xv.at[x], n_slot(r), ns_sem.at[k], nr_sem.at[r], dp(at(0, 1, 1)))
        if k == 3:
            return remote(
                xv.at[(x + 2) % NX], relay.at[c], ns_sem.at[k], rr_sem.at[c], dp(at(1 + 2 * c, 0, 1))
            )
        dx = (None, 1, 3, None, 0)[k]
        return remote(xv.at[(x + dx) % NX], n_slot(r), ns_sem.at[k], nr_sem.at[r], dp(at(dx, 0, 1)))

    for k in range(1, 16):
        f_send(k).start()

    @pl.when(value_core)
    def _():
        f_send(0).start()
        n_send(4).start()

    @pl.when(feature_core)
    def _():
        c_home.start()

    c_send(0).start()
    for k in range(1, 3):
        n_send(k).start()
    for k in range(1, 3):
        c_send(k).start()
    n_send(3).start()

    @pl.when(value_core)
    def _():
        c_slot(r)[...] = cv[y]

    @pl.when(feature_core)
    def _():
        c_slot(r)[...] = cv[y]
        n_slot(r)[...] = xv[x]
        fsq[16 * t + r] = sqs[0:8, :]

    loads[2 + NF].wait()

    def x_lanes(k, h):
        per = BLOCK // cw
        lane = pl.multiple_of((k % per) * cw + h * 128, 128)
        return xv[k // per, :, pl.ds(lane, 128)].astype(F32)

    def upstream_step(k, total):
        rows = pl.ds(pl.multiple_of(k * cw, cw), cw)
        up = dot_nt(cv[0], wv[rows, pl.ds(0, BLOCK)]) + dot_nt(cv[1], wv[rows, pl.ds(BLOCK, BLOCK)])
        up = up * gain[0:1, pl.ds(pl.multiple_of(k * cw, cw), cw)]
        scaled[k] = up
        for h in range(cw // 128):
            total = total + up[:, h * 128 : (h + 1) * 128] * x_lanes(k, h)
        return total

    inner = lax.fori_loop(0, CHUNKS, upstream_step, jnp.zeros((tok, 128), F32))
    ins[...] = as_row(inner)
    inner_copy = remote(ins, inr, small_s.at[1], small_r.at[1], partner)
    inner_copy.start()
    n_send(0).start()

    def term_ready():
        squares_copy.wait_recv()
        inner_copy.wait_recv()
        row = lax.rsqrt((sqs[0:1, :] + sqr[0:1, :]) / full + EPSILON)
        inv_v[...] = as_column(row)
        coef_v[...] = as_column(row * row * row * (ins[0:1, :] + inr[0:1, :]) / full)
        for k in range(NF):
            loads[3 + NF + k].wait()

    def z_copy(chunk):
        return remote(
            zsend.at[chunk],
            zrecv.at[chunk],
            zs_sem.at[chunk],
            zr_sem.at[chunk],
            {"section": (s + sections - 1) % sections},
        )

    def z_step(chunk):
        @pl.when(s < sections - 1)
        def _():
            z_copy(chunk).wait_recv()

        @pl.when(s == sections - 1)
        def _():
            zrecv[chunk] = jnp.zeros((tok, 128), BF16)

        up = scaled[chunk * 128 // cw, :, pl.ds(pl.multiple_of(chunk * 128 % cw, 128), 128)]
        block = chunk * 128 // BLOCK
        lanes = pl.ds(pl.multiple_of(chunk * 128 % BLOCK, 128), 128)
        term = inv_v[...] * up - xv[block, :, lanes].astype(F32) * coef_v[...]
        term = term + zrecv[chunk].astype(F32)
        zsend[chunk] = term.astype(BF16)
        columns = pl.ds(pl.multiple_of(chunk * 128, 128), 128)
        og[:, columns] = (tv[block, :, lanes].astype(F32) + term).astype(BF16)

        @pl.when(s > 0)
        def _():
            z_copy(chunk).start()

    def z_count(when):
        come = (2 * (when - 140 - (36 - 2 * c) * (sections - 1 - s)) + 3000) // 15 - 199
        come = come + LINKS * (s // (sections - 1)) * (when // 110)
        return jnp.minimum(jnp.maximum(come, 0), LINKS) * ((s + sections - 1) // sections)

    def z_point(last, now):
        def step(chunk, carry):
            z_step(chunk)
            return carry

        lax.fori_loop(z_count(last), z_count(now), step, 0)

    def z_end():
        @pl.when(s == 0)
        def _():
            def step(chunk, carry):
                z_step(chunk)
                return carry

            lax.fori_loop(0, LINKS, step, 0)

    ee[...] = jnp.zeros((BLOCK, BLOCK), F32)

    def place(k):
        high = k // 6
        return (1 - high) * (k % 3 + (k % 3) // 2) + 2 * high, (1 - high) * (k // 3) + high * (k % 2)

    def n_forward(k, core):
        index = at((0, 1, 3, 2)[k], 0, core)
        return remote(
            n_slot(index), n_slot(index), nf_sem.at[2 * k + core], nr_sem.at[index], dp(at(0, 1, 1))
        )

    def n_arrived(index):
        return remote(n_slot(index), n_slot(index), nf_sem.at[0], nr_sem.at[index], dp(at(0, 1, 1)))

    def f_arrived(index):
        return remote(fsq.at[index], fsq.at[index], fs_sem.at[0], fr_sem.at[index], dp(at(0, 1, 1)))

    def c_arrived(index):
        return remote(c_slot(index), c_slot(index), cs_sem.at[0], cr_sem.at[index], dp(at(1, 0, 0)))

    def c_back(index):
        return remote(c_slot(index), c_slot(index), cb_sem.at[index], cr_sem.at[index], dp(at(0, 0, 1)))

    def norm_slot(index):
        total = fsq[index][0:1, :] + fsq[16 + index][0:1, :]
        inverse = as_column(lax.rsqrt(total / full + EPSILON))
        rows = pl.ds(pl.multiple_of(index * tok, tok), tok)
        for h in range(BLOCK // 128):
            lanes = slice(h * 128, (h + 1) * 128)
            row = gain[0:1, pl.ds(pl.multiple_of(x * BLOCK + h * 128, 128), 128)]
            nn[rows, lanes] = (nbuf[rows, lanes].astype(F32) * inverse * row).astype(BF16)

    def n_relay(side):
        dx = (3, 1)[side]
        return remote(
            relay.at[side],
            n_slot(at(dx, 0, side)),
            rs_sem.at[side],
            nr_sem.at[at(dx, 0, side)],
            dp(at((1, 3)[side], 0, 1)),
        )

    def n_relayed(side):
        return remote(relay.at[side], relay.at[side], rs_sem.at[side], rr_sem.at[side], dp(at(1, 0, 1)))

    def pair(k):
        dx, dy = place(k)
        return pl.ds(pl.multiple_of(at(dx, dy, 0) * tok, 2 * tok), 2 * tok)

    def add_grad(k):
        dx, dy = place(k)

        @pl.when(k > 0)
        def _():
            c_arrived(at(dx, dy, 1)).wait_recv()

        c_arrived(at(dx, dy, 0)).wait_recv()
        gacc[...] = gacc[...] + dot_tn(nn[pair(k), :], cbuf[pair(k), :])

    @pl.when(feature_core)
    def _():
        gacc[...] = jnp.zeros((BLOCK, BLOCK), F32)

        def pass_on(k):
            for core in (1, 0):
                n_arrived(at((0, 1, 3, 2)[k], 0, core)).wait_recv()
                n_forward(k, core).start()

        def step_time(k):
            late = (k + 6) // 8
            return late * (172 + 13 * k) + (1 - late) * (128 + 22 * k)

        def step(k, carry):
            dx, dy = place(k)

            @pl.when(k == 1)
            def _():
                pass_on(1)
                pass_on(2)

            @pl.when(k == 2)
            def _():
                for side in range(2):
                    n_relayed(side).wait_recv()
                    n_relay(side).start()

            @pl.when(k == 4)
            def _():
                pass_on(3)

            @pl.when(((k > 2) & (k < 6)) | (k == 7))
            def _():
                n_arrived(at(dx, dy, 1)).wait_recv()

            @pl.when((k == 0) | ((k > 2) & (k < 6)) | (k == 7))
            def _():
                n_arrived(at(dx, dy, 0)).wait_recv()

            for core in (1, 0):
                index = at(dx, dy, core)
                f_arrived(index + 16 * (1 - t)).wait_recv()
                if core == 0:
                    f_arrived(index + 16 * t).wait_recv()
                else:

                    @pl.when(k > 0)
                    def _():
                        f_arrived(index + 16 * t).wait_recv()

                norm_slot(index)
            ee[...] = ee[...] + dot_tn(nn[pair(k), :], nn[pair(k), :])

            @pl.when(k == 0)
            def _():
                term_ready()

            @pl.when(k > 0)
            def _():
                add_grad(k - 1)

            z_point(step_time(k - 1), step_time(k))
            return carry

        lax.fori_loop(0, 8, step, 0)
        limit = sweeps[0, 0, owner[0, 0, x]].astype(F32)
        lim[...] = jnp.full((8, BLOCK), limit, F32)

    def c_place(k):
        low, high = (7 - k) // 6, k // 6
        middle = 1 - low - high
        dx = middle * (1 + 2 * (k % 2)) + high * 2
        dy = (low + high) * (k % 2) + middle * (k // 2 - 1)
        return dx, dy

    def c_forward(dx, dy, core, to_right, n):
        index = at(dx, dy, core)
        return remote(
            c_slot(index),
            c_slot(index),
            cs_sem.at[n],
            cr_sem.at[index],
            dp(at(1 if to_right else 3, 0, 0)),
        )

    c_forwards = {
        1: [(0, 1, core, way, 4 + 2 * core + way) for core in range(2) for way in range(2)],
        2: [(1, 0, 1, 0, 8)],
        3: [(3, 0, 0, 1, 9)],
        4: [(1, 1, 1, 0, 10)],
        5: [(3, 1, 0, 1, 11)],
    }

    @pl.when(value_core)
    def _():
        def step(k, carry):
            dx, dy = c_place(k)
            for core in (0, 1):
                if core == 1:
                    c_arrived(at(dx, dy, core)).wait_recv()
                else:

                    @pl.when(k > 0)
                    def _():
                        c_arrived(at(dx, dy, core)).wait_recv()

                if core == 0:
                    c_back(at(dx, dy, core)).start()
                else:

                    @pl.when(k > 0)
                    def _():
                        c_back(at(dx, dy, core)).start()

            for number, forwards in c_forwards.items():

                @pl.when(k == number)
                def _():
                    for forward in forwards:
                        c_forward(*forward).start()

            rows = cbuf[pl.ds(pl.multiple_of(at(dx, dy, 0) * tok, 2 * tok), 2 * tok), :]
            ee[...] = ee[...] + dot_tn(rows, rows)

            @pl.when(k == 1)
            def _():
                term_ready()

            z_point(89 + 20 * k, 109 + 20 * k)

            return carry

        lax.fori_loop(0, 8, step, 0)
        other = sqr[8:9, :]
        own = jnp.full((1, 128), own_limit, F32)
        limit = jnp.where(y == t, own, other)
        for h in range(BLOCK // 128):
            lim[:, h * 128 : (h + 1) * 128] = jnp.broadcast_to(limit, (8, 128))

    diagonal = lax.broadcasted_iota(jnp.int32, (BLOCK, BLOCK), 0) == lax.broadcasted_iota(
        jnp.int32, (BLOCK, BLOCK), 1
    )
    matrix = ee[...] / tokens + jnp.where(diagonal, DAMPING, 0.0)
    norm = lax.rsqrt(jnp.sum(jnp.sum(matrix * matrix, axis=0, keepdims=True), axis=1, keepdims=True))
    ee[...] = matrix * norm
    xx[...] = jnp.where(diagonal, 1.0, 0.0) * norm

    def sweep(k, carry):
        eb[...] = ee[...].astype(BF16)

        @pl.when(k > 0)
        def _():
            old = xx[...]
            new = 2.0 * old - dot_nn(old.astype(BF16), eb[...])
            xx[...] = jnp.where(lim[0:1, :] > k.astype(F32), new, old)

        @pl.when(k == 0)
        def _():
            xx[...] = 2.0 * xx[...] - ee[...] * norm

        @pl.when(k < ITERS - 1)
        def _():
            e = ee[...]
            ee[...] = 2.0 * e - dot_nn(eb[...], eb[...])

        @pl.when((c == 1) & (k == 2))
        def _():
            add_grad(jnp.int32(7))
            gb[...] = gacc[...].astype(BF16)

        before = (10 - 5 * c) * (1 - (k + 5) // 6)
        z_point(259 + 9 * c + 10 * k - before, 269 + 9 * c + 10 * k)

        return carry

    lax.fori_loop(0, ITERS, sweep, 0)
    eb[...] = xx[...].astype(BF16)

    v_copy = remote(eb, vb, gv_s.at[0], gv_r.at[0], dp(at(0, 0, 1)))

    @pl.when(value_core)
    def _():
        v_copy.start()

        z_point(319, 340)

    rows_q = BLOCK // 4

    def piece(dx, dy, q):
        return (((x + dx) % NX) * 2 + (y + dy) % 2) * 4 + q

    def to(dx, dy, q, n, device):
        index = piece(dx, dy, q)
        return remote(pv.at[index], pv.at[index], as_sem.at[n], ar_sem.at[index], dp(device))

    def arrived(dx, dy, q):
        return to(dx, dy, q, 0, at(0, 0, 1 - c))

    def run(events, my_core):
        started = []
        n = 0
        for dx, dy, q, arrives, goes in events:
            if arrives:
                arrived(dx, dy, q).wait_recv()
            for where in goes:
                copy = to(dx, dy, where[3] if len(where) > 3 else q, n, at(*where[:3]))
                copy.start()
                started.append(copy)
                n += 1
            yield
        for dx, dy, q in [
            (dx, dy, q)
            for dy in range(2)
            for dx in (0, 1, 3, 2)
            for q in ((2, 3) if my_core == 1 else (0, 1))
            if my_core == 0 or (dx, dy) != (0, 0)
        ]:
            arrived(dx, dy, q).wait_recv()
        for copy in started:
            copy.wait_send()

    @pl.when(feature_core)
    def _():
        right, left, up, across = (1, 0, 1), (3, 0, 1), (0, 1, 1), (0, 0, 0)
        z_point(328, 340)
        lb[...] = dot_nn(eb[...], gb[...]).astype(BF16)
        v_copy.wait_recv()
        events = [
            (0, 0, 0, False, (right, up, across)),
            (0, 0, 2, False, ((0, 1, 0), across)),
            (0, 0, 1, False, (left, left + (0,), right, up, across)),
            (0, 0, 3, False, ((0, 1, 0), across)),
        ]
        events += [
            (3, 0, 0, True, (right, up, across)),
            (1, 0, 1, True, (left, up, across)),
            (0, 1, 0, True, (across,)),
            (3, 0, 1, True, (up, across)),
            (1, 0, 0, True, (up, across)),
            (0, 1, 1, True, (across,)),
            (2, 0, 0, True, (up, across)),
            (2, 0, 1, True, (up, across)),
            (3, 1, 0, True, (across,)),
            (1, 1, 1, True, (across,)),
            (3, 1, 1, True, (across,)),
            (1, 1, 0, True, (across,)),
            (2, 1, 0, True, (across,)),
            (2, 1, 1, True, (across,)),
        ]
        steps = run(events, 1)
        for q in (0, 2, 1, 3):
            rows = slice(q * rows_q, (q + 1) * rows_q)
            pv[piece(0, 0, q)] = dot_nn(lb[rows, :], vb[...]).astype(BF16)
            next(steps)
        z_point(340, 380)
        time = 380
        times = (408, 424, 432, 444, 458, 472, 486, 495, 500, 505, 510, 515, 520, 9000)
        for number in range(len(events) - 4):
            next(steps)
            now = times[number]
            z_point(time, now)
            time = now
        z_end()
        for _ in steps:
            pass

    @pl.when(value_core)
    def _():
        right, left, across = (1, 0, 0), (3, 0, 0), (0, 0, 1)
        events = [
            (0, 0, 2, True, (right,)),
            (0, 1, 2, True, (right, across)),
            (0, 0, 3, True, (left, left + (2,), right)),
            (0, 1, 3, True, (left, left + (2,), right, across)),
            (3, 0, 2, True, (right, across)),
            (1, 0, 3, True, (left, across)),
            (3, 1, 2, True, (right, across)),
            (1, 1, 3, True, (left, across)),
            (3, 0, 3, True, (across,)),
            (1, 0, 2, True, (across,)),
            (3, 1, 3, True, (across,)),
            (1, 1, 2, True, (across,)),
            (2, 0, 2, True, (across,)),
            (2, 0, 3, True, (across,)),
            (2, 1, 2, True, (across,)),
            (2, 1, 3, True, (across,)),
        ]
        steps = run(events, 0)
        time = 340
        times = (365, 368, 390, 400, 415, 426, 437, 445, 452, 460, 467, 476, 485, 493, 500, 9000)
        for number in range(len(events)):
            next(steps)
            now = times[number]
            z_point(time, now)
            time = now
        z_end()
        for _ in steps:
            pass

    squares_copy.wait_send()
    inner_copy.wait_send()
    for k in range(3):
        c_send(k).wait_send()
    for k in range(4):
        n_send(k).wait_send()
    for k in range(1, 16):
        f_send(k).wait_send()

    @pl.when(feature_core)
    def _():
        c_home.wait_send()
        for side in range(2):
            n_relay(side).wait_send()

        for k in range(1, 4):
            for core in range(2):
                n_forward(k, core).wait_send()

    @pl.when(value_core)
    def _():
        f_send(0).wait_send()
        n_send(4).wait_send()

        def ended(k, carry):
            dx, dy = place(k)
            c_back(at(dx, dy, 0)).wait_send()

            @pl.when(k > 0)
            def _():
                c_back(at(dx, dy, 1)).wait_send()

            return carry

        lax.fori_loop(0, 8, ended, 0)
        for forwards in c_forwards.values():
            for forward in forwards:
                c_forward(*forward).wait_send()
        v_copy.wait_send()

    def chain_ended(chunk, carry):
        @pl.when(s > 0)
        def _():
            z_copy(chunk).wait_send()

        return carry

    lax.fori_loop(0, LINKS, chain_ended, 0)


def lay_out(grad, pieces, grad_out, pre_out, grad_sem, pre_sem):
    copies = []
    rows = pieces.shape[1]
    for n in range(32):
        i, j, q = n // 8, (n // 4) % 2, n % 4
        out = pre_out.at[0, pl.ds(i * BLOCK + q * rows, rows), pl.ds(j * BLOCK, BLOCK)]
        copies.append(pltpu.make_async_copy(pieces.at[n], out, pre_sem.at[n]))
    copies.append(pltpu.make_async_copy(grad, grad_out.at[0], grad_sem.at[0]))
    for copy in copies:
        copy.start()
    for copy in copies:
        copy.wait()


def on_device(sections, tokens, activations, norm_gain, weights, cotangent, top_grad, owner_slot, sweeps):
    tok, half_width = activations.shape[1:]
    value_width = weights.shape[2]
    cw = half_width // CHUNKS
    vmem = functools.partial(pltpu.VMEM)
    dma = pltpu.SemaphoreType.DMA
    anywhere = pl.BlockSpec(memory_space=pl.ANY)
    hbm = pl.BlockSpec(memory_space=pltpu.HBM)
    smem = pl.BlockSpec(memory_space=pltpu.SMEM)
    grad, pieces = pl.pallas_call(
        functools.partial(kernel, sections, tokens),
        out_shape=(
            pltpu.VMEM((tok, half_width), BF16),
            pltpu.VMEM((32, BLOCK // 4, BLOCK), BF16),
        ),
        in_specs=[
            smem,
            smem,
            hbm,
            pl.BlockSpec(memory_space=pltpu.VMEM),
            hbm,
            hbm,
            hbm,
        ],
        out_specs=(pl.BlockSpec(memory_space=pltpu.VMEM),) * 2,
        scratch_shapes=[
            vmem((NF, tok, BLOCK), BF16),
            vmem((2, tok, BLOCK), BF16),
            vmem((half_width, value_width), BF16),
            vmem((NF, tok, BLOCK), BF16),
            vmem((CHUNKS, tok, cw), F32),
            vmem((tok * 16, BLOCK), BF16),
            vmem((tok * 16, BLOCK), BF16),
            vmem((tok * 16, BLOCK), BF16),
            vmem((BLOCK, BLOCK), F32),
            vmem((32, 8, 128), F32),
            vmem((BLOCK, BLOCK), F32),
            vmem((BLOCK, BLOCK), F32),
            vmem((BLOCK, BLOCK), BF16),
            vmem((BLOCK, BLOCK), BF16),
            vmem((BLOCK, BLOCK), BF16),
            vmem((BLOCK, BLOCK), BF16),
            vmem((16, 128), F32),
            vmem((16, 128), F32),
            vmem((8, 128), F32),
            vmem((8, 128), F32),
            vmem((tok, 128), F32),
            vmem((tok, 128), F32),
            vmem((8, BLOCK), F32),
            vmem((LINKS, tok, 128), BF16),
            vmem((LINKS, tok, 128), BF16),
            vmem((2, tok, BLOCK), BF16),
            dma((3 + 2 * NF,)),
            dma((12,)),
            dma((16,)),
            dma((16,)),
            dma((16,)),
            dma((32,)),
            dma((5,)),
            dma((8,)),
            dma((16,)),
            dma((2,)),
            dma((2,)),
            dma((2,)),
            dma((2,)),
            dma((LINKS,)),
            dma((LINKS,)),
            dma((1,)),
            dma((1,)),
            dma((40,)),
            dma((32,)),
        ],
        compiler_params=pltpu.CompilerParams(
            collective_id=0, has_side_effects=True, vmem_limit_bytes=60000 * 1024
        ),
        name="kfac",
    )(owner_slot, sweeps, activations, norm_gain, weights, cotangent, top_grad)
    return pl.pallas_call(
        lay_out,
        out_shape=(
            jax.ShapeDtypeStruct((1, tok, half_width), BF16),
            jax.ShapeDtypeStruct((1, half_width, value_width), BF16),
        ),
        in_specs=[anywhere, anywhere],
        out_specs=(anywhere, anywhere),
        scratch_shapes=[dma((1,)), dma((32,))],
        compiler_params=pltpu.CompilerParams(vmem_limit_bytes=1 << 20),
        name="lay_out",
    )(grad, pieces)


def solution(mesh):
    sections = mesh.shape["section"]
    placed = (
        P("section", "dp", "tensor"),
        P("section", "tensor"),
        P("section", "tensor", None),
        P("section", "dp", None),
        P("dp", "tensor"),
        P("section", "tensor", None),
        P("section", "tensor", None),
    )

    def step(activations, *rest):
        return on_device(sections, activations.shape[1] * 16, activations, *rest)

    return jax.shard_map(
        step,
        mesh=mesh,
        in_specs=placed,
        out_specs=(P("section", "dp", "tensor"), P("section", "tensor", None)),
        check_vma=False,
    )
```
